32 devices in a mesh: bins: 4 (over x, core), sta: 8 (over z, y).
Axes of the slice: x: 2, y: 2, z: 4, core: 2. Of those that a mesh axis runs over, the one named last changes fastest.
Arguments:
- spectra: bfloat16 [2, 128, 8, 2048], P(None, 'bins', None, 'sta'), may hold values from -110 to 110
- coords: int32 [2, 2048], replicated, may hold values from 0 to 2047
- slowness: int32 [2, 2048], replicated, may hold values from -32 to 31
Outputs:
- beam_power: float32 [128, 2048], P('bins', 'sta')
The draws below stay inside these ranges and needn't reach their ends.
All inputs are finite; a program needn't handle non-finite values.
Results may differ from the reference program's by a relative error of at most 0.002.
Values may be sent and summed in bfloat16 or wider, within the bound.
A program may use at most 64 MiB of HBM per device.

```python
import math
import jax
import jax.numpy as jnp
from jax import lax

FREQS = 128
BEAMS = 2048
SEGS = 8
STATIONS = 2048


def draw_spectra(key, part):
    keys = jax.random.split(key, 3)
    levels = jnp.arange(FREQS, dtype=jnp.float32) / FREQS
    tilt = jnp.exp(jnp.log(4.0) * levels)
    seg_gain = jax.random.uniform(keys[1], (SEGS,), jnp.float32, 0.5, 1.5)
    noise = jnp.clip(jax.random.normal(keys[0], (2, FREQS, SEGS, STATIONS), jnp.float32), -3.0, 3.0)
    station_gain = jnp.exp(jax.random.uniform(keys[2], (STATIONS,), jnp.float32, jnp.log(0.5), jnp.log(2.0)))
    values = noise * tilt[None, :, None, None] * seg_gain[None, None, :, None] * station_gain[None, None, None, :]
    return values.astype(jnp.bfloat16)


def plant(entries, key, least, top_value):
    spot = [jax.random.randint(jax.random.fold_in(key, axis), (), 0, length) for axis, length in enumerate(entries.shape)]
    widest = entries.shape.index(max(entries.shape))
    next_to = spot[:widest] + [(spot[widest] + 1) % entries.shape[widest]] + spot[widest + 1:]
    return entries.at[tuple(spot)].set(least).at[tuple(next_to)].set(top_value)


def setup_inputs(seed: int = 0) -> dict:
    seeds = jax.random.split(jax.random.key(seed), 4)
    spectra = draw_spectra(jax.random.fold_in(seeds[3], 71), 0)
    coords = plant(jax.random.randint(seeds[1], (2, STATIONS), 0, 2048), jax.random.fold_in(seeds[1], 1), 0, 2047).astype(jnp.int32)
    slowness = plant(jax.random.randint(seeds[2], (2, BEAMS), -32, 32), jax.random.fold_in(seeds[2], 1), -32, 31).astype(jnp.int32)
    return {"spectra": spectra, "coords": coords, "slowness": slowness}


phase_modulus = 1048576
two_pi = 2.0 * math.pi
epsilon = 1e-06

def steering_table(delays, bin_number):
    phase_index = jnp.mod(bin_number * delays, phase_modulus)
    phase = phase_index.astype(jnp.float32) * (two_pi / phase_modulus)
    return jnp.concatenate([jnp.cos(phase), jnp.sin(phase)], 0).astype(jnp.bfloat16)

def reference(spectra, coords, slowness):
    values = spectra.astype(jnp.float32)
    sumsq = lax.optimization_barrier(jnp.sum(values * values, axis=(0, 1)))
    scale = jnp.sqrt(sumsq / (2 * FREQS) + epsilon)
    whitened = (values / scale).astype(jnp.bfloat16)
    delays = slowness[0][None, :] * coords[0][:, None] + slowness[1][None, :] * coords[1][:, None]

    def one_bin(pair_args):
        bin_white, bin_number = pair_args
        real_part = bin_white[0]
        imag_part = bin_white[1]
        upper_rows = jnp.concatenate([real_part, imag_part], 1)
        bottom = jnp.concatenate([imag_part, -imag_part * 0 - real_part], 1)
        stacked = jnp.concatenate([upper_rows, bottom], 0).astype(jnp.float32)
        steering = steering_table(delays, bin_number).astype(jnp.float32)
        amplitude = jnp.dot(stacked, steering, preferred_element_type=jnp.float32)
        return lax.optimization_barrier(jnp.sum(amplitude * amplitude, axis=0))
    bin_numbers = jnp.arange(1, FREQS + 1, dtype=jnp.int32)
    beam_power = lax.map(one_bin, (jnp.moveaxis(whitened, 1, 0), bin_numbers))
    return beam_power / (STATIONS * SEGS)
```

```python
import functools
import math

import jax
import jax.numpy as jnp
from jax import lax
from jax.experimental import pallas as pl
from jax.experimental.pallas import tpu as pltpu
from jax.sharding import PartitionSpec as P

epsilon = 1e-06
MESH = pl.DeviceIdType.MESH

SIN_COEFS = (6.28318501, -41.3415909, 81.5999451, -76.6144714, 41.3428841, -12.4712439)
COS_COEFS = (1.0, -19.7392044, 64.9391174, -85.4501419, 60.1676292, -25.9675999, 6.52865839)


def horner(coefs, z):
    acc = jnp.full_like(z, coefs[-1])
    for c in coefs[-2::-1]:
        acc = acc * z + c
    return acc


def cos_sin(index):
    turns = (index << 11).astype(jnp.float32) * (2.0 ** -32)
    z = turns * turns
    return horner(COS_COEFS, z), horner(SIN_COEFS, z) * turns


def kernel(
    dims,
    spectra,
    coords_hbm,
    slowness_hbm,
    out,
    coords,
    slowness,
    own,
    blocks,
    squares,
    scales,
    cos_b,
    sin_b,
    rotor,
    right,
    left,
    product,
    grid_hi_lo,
    onehot,
    picked,
    returned,
    own_sem,
    local_sem,
    coords_sem,
    slow_sem,
    sq_send,
    sq_recv,
    sc_send,
    sc_recv,
    bl_send,
    bl_recv,
    re_send,
    re_recv,
):
    n_bins, n_sta, groups, copies, fb, bins_dev, segs, sta_dev, beams_dev = dims
    me = lax.axis_index("sta")
    mb = lax.axis_index("bins")
    group = me // copies
    lane_of = me % copies
    f32, bf16 = jnp.float32, jnp.bfloat16

    def partner(o):
        if n_sta & (n_sta - 1):
            return (me + o) % n_sta
        return me ^ o

    def origin(o):
        if n_sta & (n_sta - 1):
            return (me - o + n_sta) % n_sta
        return me ^ o

    own_copy = pltpu.make_async_copy(spectra, own, own_sem)
    own_copy.start()
    local_copy = pltpu.make_async_copy(
        spectra.at[:, pl.ds(group * fb, fb)], blocks.at[me], local_sem
    )
    local_copy.start()
    coords_copy = pltpu.make_async_copy(coords_hbm, coords, coords_sem)
    coords_copy.start()
    slow_copy = pltpu.make_async_copy(slowness_hbm, slowness, slow_sem)
    slow_copy.start()

    barrier = pltpu.get_barrier_semaphore()
    for o in range(1, n_bins):
        pl.semaphore_signal(
            barrier, inc=1, device_id={"bins": (mb + o) % n_bins}, device_id_type=MESH
        )
    for o in range(1, n_sta):
        pl.semaphore_signal(
            barrier, inc=1, device_id={"sta": partner(o)}, device_id_type=MESH
        )

    own_copy.wait()

    def square_step(f, acc):
        re = own[0, f].astype(f32)
        im = own[1, f].astype(f32)
        return acc + re * re + im * im

    squares[mb] = lax.fori_loop(
        0, bins_dev, square_step, jnp.zeros((segs, sta_dev), f32), unroll=True
    )

    coords_copy.wait()
    first_bin = mb * bins_dev + group * fb + 1

    def table_step(step, carry):
        f = step // n_sta
        at = pl.ds(pl.multiple_of((step % n_sta) * sta_dev, sta_dev), sta_dev)
        bin_number = first_bin + f
        east = coords[0:1, at] * bin_number
        north = coords[1:2, at] * bin_number
        ids = lax.broadcasted_iota(jnp.int32, (8, sta_dev), 0)
        cb, sb = cos_sin((2 * ids + 1) * east)
        cos_b[f, :, at] = cb
        sin_b[f, :, at] = sb
        steps = jnp.where(ids == 0, 16, jnp.where(ids == 1, 48, 1))
        ca, sa = cos_sin(steps * east + jnp.where(ids == 2, north, 0))
        rotor[f, 0, :, at] = ca
        rotor[f, 1, :, at] = sa
        ids = lax.broadcasted_iota(jnp.int32, (16, sta_dev), 0)
        for half in range(2):
            cy, sy = cos_sin((2 * ids + (32 * half + 1)) * north)
            for a in range(2):
                c, s = ca[a : a + 1], sa[a : a + 1]
                cc, ss, sc, cs = c * cy, s * sy, s * cy, c * sy
                base = a * 64 + half * 16
                right[f, base : base + 16, at] = (cc - ss).astype(bf16)
                right[f, base + 32 : base + 48, at] = (cc + ss).astype(bf16)
                right[f, base + 128 : base + 144, at] = (sc + cs).astype(bf16)
                right[f, base + 160 : base + 176, at] = (sc - cs).astype(bf16)
        return carry

    lax.fori_loop(0, fb * n_sta // 2, table_step, 0)
    product[...] = jnp.zeros_like(product)

    slow_copy.wait()
    sx = slowness[0:1, :] + 32
    sy = slowness[1:2, :] + 32
    a_index = sx // 16
    flipped = a_index < 2
    y_index = jnp.where(flipped, 63 - sy, sy)
    y_slot = jnp.where(y_index >= 32, y_index - 32, 63 - y_index)
    a_slot = jnp.where(flipped, 1 - a_index, a_index - 2)
    column = jnp.where(flipped, 128, 0) + a_slot * 64 + y_slot
    for i in range(16):
        ids = lax.broadcasted_iota(jnp.int32, (16, column.shape[1]), 0) + 16 * i
        onehot[i * 16 : (i + 1) * 16, :] = jnp.where(ids == column, 1.0, 0.0).astype(bf16)

    pl.semaphore_wait(barrier, n_bins + n_sta - 2)

    def square_send(o):
        return pltpu.make_async_remote_copy(
            src_ref=squares.at[mb],
            dst_ref=squares.at[mb],
            send_sem=sq_send.at[o],
            recv_sem=sq_recv.at[mb],
            device_id={"bins": (mb + o) % n_bins},
            device_id_type=MESH,
        )

    def square_arrival(o):
        source = (mb + o) % n_bins
        return pltpu.make_async_remote_copy(
            src_ref=squares.at[source],
            dst_ref=squares.at[source],
            send_sem=sq_send.at[o],
            recv_sem=sq_recv.at[source],
            device_id={"bins": source},
            device_id_type=MESH,
        )

    def scale_send(o):
        return pltpu.make_async_remote_copy(
            src_ref=scales.at[me],
            dst_ref=scales.at[me],
            send_sem=sc_send.at[o],
            recv_sem=sc_recv.at[me],
            device_id={"sta": partner(o)},
            device_id_type=MESH,
        )

    def scale_arrival(o):
        source = origin(o)
        return pltpu.make_async_remote_copy(
            src_ref=scales.at[source],
            dst_ref=scales.at[source],
            send_sem=sc_send.at[o],
            recv_sem=sc_recv.at[source],
            device_id={"sta": source},
            device_id_type=MESH,
        )

    def block_send(o):
        target = partner(o)
        return pltpu.make_async_remote_copy(
            src_ref=own.at[:, pl.ds((target // copies) * fb, fb)],
            dst_ref=blocks.at[me],
            send_sem=bl_send.at[o],
            recv_sem=bl_recv.at[me],
            device_id={"sta": target},
            device_id_type=MESH,
        )

    def block_arrival(o):
        source = origin(o)
        return pltpu.make_async_remote_copy(
            src_ref=blocks.at[source],
            dst_ref=blocks.at[source],
            send_sem=bl_send.at[o],
            recv_sem=bl_recv.at[source],
            device_id={"sta": source},
            device_id_type=MESH,
        )

    for o in range(1, n_bins):
        square_send(o).start()
    for o in range(n_sta - 1, 0, -1):
        block_send(o).start()

    lax.fori_loop(fb * n_sta // 2, fb * n_sta, table_step, 0)
    for o in range(1, n_bins):
        square_arrival(o).wait_recv()
    total = squares[0]
    for b in range(1, n_bins):
        total = total + squares[b]
    scales[me] = 1.0 / jnp.sqrt(total / (2 * bins_dev * n_bins) + epsilon)
    for o in range(1, n_sta):
        scale_send(o).start()

    local_copy.wait()

    def fill(o, source):
        at = pl.ds(pl.multiple_of(source * sta_dev, sta_dev), sta_dev)
        inverse = scales[source]
        for f in range(fb):
            re = (blocks[source, 0, f].astype(f32) * inverse).astype(bf16).astype(f32)
            im = (blocks[source, 1, f].astype(f32) * inverse).astype(bf16).astype(f32)
            c0 = rotor[f, 0, 2:3, at]
            s0 = rotor[f, 1, 2:3, at]
            parts = (re * c0 - im * s0, im * c0 + re * s0)
            trig = (cos_b[f, :, at], sin_b[f, :, at])
            for p in range(2):
                for ri in range(2):
                    for g in range(0, segs, 2):
                        both = jnp.concatenate(
                            [parts[ri][g : g + 1] * trig[p], parts[ri][g + 1 : g + 2] * trig[p]], 0
                        )
                        base = ((p * 2 + ri) * segs + g) * 8
                        left[f, base : base + 16, :] = both.astype(bf16)
            product[f] += lax.dot_general(
                left[f], right[f, :, at], (((1,), (1,)), ((), ())), preferred_element_type=f32
            )

    def arrive_step(o, carry):
        @pl.when(o > 0)
        def _():
            block_arrival(o).wait_recv()
            scale_arrival(o).wait_recv()

        fill(o, origin(o))
        return carry

    lax.fori_loop(0, n_sta, arrive_step, 0)

    part = segs * 8

    def bin_power(f, carry):
        sums = [None] * 4
        for g in range(segs):
            r0 = g * 8
            ccr, csr = product[f, r0 : r0 + 8, :128], product[f, r0 : r0 + 8, 128:]
            r0 += part
            cci, csi = product[f, r0 : r0 + 8, :128], product[f, r0 : r0 + 8, 128:]
            r0 += part
            scr, ssr = product[f, r0 : r0 + 8, :128], product[f, r0 : r0 + 8, 128:]
            r0 += part
            sci, ssi = product[f, r0 : r0 + 8, :128], product[f, r0 : r0 + 8, 128:]
            pr, pi, mr, mi = ccr - ssr, cci - ssi, ccr + ssr, cci + ssi
            tr, ti, dr, di = scr + csr, sci + csi, scr - csr, sci - csi
            amps = (
                (pr + ti, pi - tr),
                (mr + di, mi - dr),
                (mr - di, mi + dr),
                (pr - ti, pi + tr),
            )
            for c, (x, y) in enumerate(amps):
                power = x * x + y * y
                sums[c] = power if sums[c] is None else sums[c] + power
        grid = jnp.concatenate(
            [jnp.concatenate(sums[0:2], 1), jnp.concatenate(sums[2:4], 1)], 0
        )
        hi = grid.astype(bf16)
        lo = (grid - hi.astype(f32)).astype(bf16)
        grid_hi_lo[0, f] = hi
        grid_hi_lo[1, f] = lo
        return carry

    lax.fori_loop(0, fb, bin_power, 0)

    norm = 1.0 / (n_sta * sta_dev * segs)
    rows = jnp.concatenate(
        [grid_hi_lo[h, f] for h in range(2) for f in range(fb)], 0
    )

    def result_send(o):
        target = ((group + o) % groups) * copies + lane_of
        return pltpu.make_async_remote_copy(
            src_ref=picked.at[target],
            dst_ref=returned.at[group],
            send_sem=re_send.at[o],
            recv_sem=re_recv.at[group],
            device_id={"sta": target},
            device_id_type=MESH,
        )

    def result_arrival(o):
        source = (group + o) % groups
        return pltpu.make_async_remote_copy(
            src_ref=returned.at[source],
            dst_ref=returned.at[source],
            send_sem=re_send.at[o],
            recv_sem=re_recv.at[source],
            device_id={"sta": source * copies + lane_of},
            device_id_type=MESH,
        )

    ids16 = lax.broadcasted_iota(jnp.int32, (16, beams_dev), 0)
    packed_rows = 16 * fb
    place = returned.at[group]
    for o in list(range(1, groups)) + [0]:
        target = ((group + o) % groups) * copies + lane_of
        at = pl.ds(pl.multiple_of(target * beams_dev, beams_dev), beams_dev)
        values = jnp.dot(rows, onehot[:, at], preferred_element_type=f32)
        values = values[:packed_rows] + values[packed_rows:]
        sx_at = slowness[0:1, at] + 32
        b_at = sx_at % 16
        row_at = jnp.where(b_at >= 8, b_at - 8, 15 - b_at)
        keep = jnp.where(ids16 == row_at, norm, 0.0)
        for f in range(fb):
            line = jnp.sum(values[f * 16 : (f + 1) * 16] * keep, axis=0, keepdims=True)
            if o:
                picked[target, f : f + 1, :] = line
            else:
                place[f : f + 1, :] = line
        if o:
            result_send(o).start()

    for o in range(1, groups):
        result_arrival(o).wait_recv()
    for g in range(groups):
        out[g * fb : (g + 1) * fb, :] = returned[g]

    for o in range(1, n_bins):
        square_send(o).wait_send()
    for o in range(1, n_sta):
        block_send(o).wait_send()
        scale_send(o).wait_send()
    for o in range(1, groups):
        result_send(o).wait_send()


def solution(mesh):
    n_bins, n_sta = mesh.shape["bins"], mesh.shape["sta"]

    def local(spectra, coords, slowness):
        _, bins_dev, segs, sta_dev = spectra.shape
        stations, beams = coords.shape[1], slowness.shape[1]
        beams_dev = beams // n_sta
        groups = math.gcd(bins_dev, n_sta)
        copies = n_sta // groups
        fb = bins_dev // groups
        dims = (n_bins, n_sta, groups, copies, fb, bins_dev, segs, sta_dev, beams_dev)
        f32, bf16 = jnp.float32, jnp.bfloat16
        dma = pltpu.SemaphoreType.DMA
        return pl.pallas_call(
            functools.partial(kernel, dims),
            out_shape=pltpu.VMEM((bins_dev, beams_dev), f32),
            in_specs=[
                pl.BlockSpec(memory_space=pltpu.HBM),
                pl.BlockSpec(memory_space=pltpu.HBM),
                pl.BlockSpec(memory_space=pltpu.HBM),
            ],
            out_specs=pl.BlockSpec(memory_space=pltpu.VMEM),
            scratch_shapes=[
                pltpu.VMEM((2, stations), jnp.int32),
                pltpu.VMEM((2, beams), jnp.int32),
                pltpu.VMEM((2, bins_dev, segs, sta_dev), bf16),
                pltpu.VMEM((n_sta, 2, fb, segs, sta_dev), bf16),
                pltpu.VMEM((n_bins, segs, sta_dev), f32),
                pltpu.VMEM((n_sta, segs, sta_dev), f32),
                pltpu.VMEM((fb, 8, stations), f32),
                pltpu.VMEM((fb, 8, stations), f32),
                pltpu.VMEM((fb, 2, 8, stations), f32),
                pltpu.VMEM((fb, 256, stations), bf16),
                pltpu.VMEM((fb, 32 * segs, sta_dev), bf16),
                pltpu.VMEM((fb, 32 * segs, 256), f32),
                pltpu.VMEM((2, fb, 16, 256), bf16),
                pltpu.VMEM((256, beams), bf16),
                pltpu.VMEM((n_sta, fb, beams_dev), f32),
                pltpu.VMEM((groups, fb, beams_dev), f32),
                dma,
                dma,
                dma,
                dma,
                dma((n_bins,)),
                dma((n_bins,)),
                dma((n_sta,)),
                dma((n_sta,)),
                dma((n_sta,)),
                dma((n_sta,)),
                dma((groups,)),
                dma((groups,)),
            ],
            compiler_params=pltpu.CompilerParams(
                collective_id=0,
                has_side_effects=True,
                vmem_limit_bytes=33554432,
            ),
            name="beam_power",
        )(*(pltpu.with_memory_space_constraint(x, pltpu.HBM) for x in (spectra, coords, slowness)))

    in_specs = (P(None, "bins", None, "sta"), P(), P())
    out_specs = P("bins", "sta")
    return jax.shard_map(local, mesh=mesh, in_specs=in_specs, out_specs=out_specs, check_vma=False)
```

```python
import functools
import math

import jax
import jax.numpy as jnp
from jax import lax
from jax.experimental import pallas as pl
from jax.experimental.pallas import tpu as pltpu
from jax.sharding import PartitionSpec as P

epsilon = 1e-06
MESH = pl.DeviceIdType.MESH

SIN_COEFS = (6.28318501, -41.3415909, 81.5999451, -76.6144714, 41.3428841, -12.4712439)
COS_COEFS = (1.0, -19.7392044, 64.9391174, -85.4501419, 60.1676292, -25.9675999, 6.52865839)


def horner(coefs, z):
    acc = jnp.full_like(z, coefs[-1])
    for c in coefs[-2::-1]:
        acc = acc * z + c
    return acc


def cos_sin(index):
    turns = (index << 11).astype(jnp.float32) * (2.0 ** -32)
    z = turns * turns
    return horner(COS_COEFS, z), horner(SIN_COEFS, z) * turns


def kernel(
    dims,
    spectra,
    coords_hbm,
    slowness_hbm,
    out,
    coords,
    slowness,
    own,
    white,
    blocks,
    squares,
    scales,
    cos_b,
    sin_b,
    rotor,
    right,
    turned,
    left,
    product,
    grid_hi_lo,
    onehot,
    picked,
    returned,
    entered,
    own_sem,
    coords_sem,
    slow_sem,
    sq_send,
    sq_recv,
    sc_send,
    sc_recv,
    bl_send,
    bl_recv,
    re_send,
    re_recv,
):
    n_bins, n_sta, groups, copies, fb, bins_dev, segs, sta_dev, beams_dev = dims
    me = lax.axis_index("sta")
    mb = lax.axis_index("bins")
    group = me // copies
    lane_of = me % copies
    f32, bf16 = jnp.float32, jnp.bfloat16

    paired = n_sta >= 4 and n_sta & (n_sta - 1) == 0
    half = n_sta // 2
    upper = me // half if paired else 0

    edge = n_sta // 4
    raw = 2 if paired else 0

    def partner(k):
        if not paired:
            return (me + k + 1) % n_sta
        flip = me & 1
        if k < 2:
            early = half - 2 + k
        elif k < half:
            early = me ^ k ^ flip
        elif k < n_sta - 2:
            early = k - half
        else:
            early = me ^ 1 ^ flip
        outer = n_sta - 2 if k == 0 else (n_sta - 1 if k == half - 1 else half + k - 1)
        if k < half:
            late = jnp.where(me < edge, outer, n_sta - 1 - k)
        else:
            late = me ^ (k - half + 2 if k < n_sta - 2 else 1) ^ flip
        return jnp.where(upper == 1, early, late) ^ flip

    def origin(k):
        if not paired:
            return (me - k - 1 + n_sta) % n_sta
        inner = jnp.logical_and(me >= edge, me < half)
        far = jnp.where(inner, k - 1, k - (half - 1))
        aside = jnp.where(jnp.logical_and(inner, k > 0), k - half + 1, k + 1)
        return jnp.where(
            jnp.logical_and(far >= 0, far < half), (1 - upper) * half + far, me ^ aside
        )

    sends_raw = upper == 1

    def is_raw(source):
        return jnp.logical_and(
            source // half == 1, jnp.logical_and(me >= half - 2, me < half)
        )

    own_copy = pltpu.make_async_copy(spectra, own, own_sem)
    own_copy.start()
    coords_copy = pltpu.make_async_copy(coords_hbm, coords, coords_sem)
    coords_copy.start()
    slow_copy = pltpu.make_async_copy(slowness_hbm, slowness, slow_sem)
    slow_copy.start()

    barrier = pltpu.get_barrier_semaphore()
    for o in range(1, n_bins):
        pl.semaphore_signal(
            barrier, inc=1, device_id={"bins": (mb + o) % n_bins}, device_id_type=MESH
        )
    for o in range(1, n_sta):
        later = me + o

        @pl.when(later < n_sta)
        def _():
            pl.semaphore_signal(
                barrier, inc=1, device_id={"sta": later}, device_id_type=MESH
            )

    own_copy.wait()

    def square_step(f, acc):
        re = own[0, f].astype(f32)
        im = own[1, f].astype(f32)
        return acc + re * re + im * im

    squares[mb] = lax.fori_loop(
        0, bins_dev, square_step, jnp.zeros((segs, sta_dev), f32), unroll=True
    )

    pl.semaphore_wait(barrier, n_bins - 1 + me)
    for o in range(1, n_sta):
        earlier = me - o

        @pl.when(earlier >= 0)
        def _():
            pl.semaphore_signal(
                entered.at[me], inc=1, device_id={"sta": earlier}, device_id_type=MESH
            )


    def square_send(o):
        return pltpu.make_async_remote_copy(
            src_ref=squares.at[mb],
            dst_ref=squares.at[mb],
            send_sem=sq_send.at[o],
            recv_sem=sq_recv.at[mb],
            device_id={"bins": (mb + o) % n_bins},
            device_id_type=MESH,
        )

    def square_arrival(o):
        source = (mb + o) % n_bins
        return pltpu.make_async_remote_copy(
            src_ref=squares.at[source],
            dst_ref=squares.at[source],
            send_sem=sq_send.at[o],
            recv_sem=sq_recv.at[source],
            device_id={"bins": source},
            device_id_type=MESH,
        )

    def scale_send(k):
        return pltpu.make_async_remote_copy(
            src_ref=scales.at[me],
            dst_ref=scales.at[me],
            send_sem=sc_send.at[k],
            recv_sem=sc_recv.at[me],
            device_id={"sta": partner(k)},
            device_id_type=MESH,
        )

    def scale_arrival(source):
        return pltpu.make_async_remote_copy(
            src_ref=scales.at[source],
            dst_ref=scales.at[source],
            send_sem=sc_send.at[0],
            recv_sem=sc_recv.at[source],
            device_id={"sta": source},
            device_id_type=MESH,
        )

    def block_send(k, values):
        target = partner(k)
        return pltpu.make_async_remote_copy(
            src_ref=values.at[:, pl.ds((target // copies) * fb, fb)],
            dst_ref=blocks.at[me],
            send_sem=bl_send.at[k],
            recv_sem=bl_recv.at[me],
            device_id={"sta": target},
            device_id_type=MESH,
        )

    def await_entry(k):
        target = partner(k)

        @pl.when(target > me)
        def _():
            pl.semaphore_wait(entered.at[target], 1)

    def block_arrival(source):
        return pltpu.make_async_remote_copy(
            src_ref=blocks.at[source],
            dst_ref=blocks.at[source],
            send_sem=bl_send.at[0],
            recv_sem=bl_recv.at[source],
            device_id={"sta": source},
            device_id_type=MESH,
        )

    for o in range(1, n_bins):
        square_send(o).start()
    if raw:

        @pl.when(sends_raw)
        def _():
            for k in range(raw):
                await_entry(k)
                block_send(k, own).start()


    coords_copy.wait()
    first_bin = mb * bins_dev + group * fb + 1

    def table_step(step, carry):
        f = step // n_sta
        at = pl.ds(pl.multiple_of((step % n_sta) * sta_dev, sta_dev), sta_dev)
        bin_number = first_bin + f
        east = coords[0:1, at] * bin_number
        north = coords[1:2, at] * bin_number
        ids = lax.broadcasted_iota(jnp.int32, (8, sta_dev), 0)
        cb, sb = cos_sin((2 * ids + 1) * east)
        cos_b[f, :, at] = cb
        sin_b[f, :, at] = sb
        steps = jnp.where(ids == 0, 16, jnp.where(ids == 1, 48, 1))
        ca, sa = cos_sin(steps * east + jnp.where(ids == 2, north, 0))
        rotor[f, 0, :, at] = ca
        rotor[f, 1, :, at] = sa
        ids = lax.broadcasted_iota(jnp.int32, (16, sta_dev), 0)
        for half in range(2):
            cy, sy = cos_sin((2 * ids + (32 * half + 1)) * north)
            for a in range(2):
                c, s = ca[a : a + 1], sa[a : a + 1]
                cc, ss, sc, cs = c * cy, s * sy, s * cy, c * sy
                base = a * 64 + half * 16
                right[f, base : base + 16, at] = (cc - ss).astype(bf16)
                right[f, base + 32 : base + 48, at] = (cc + ss).astype(bf16)
                right[f, base + 128 : base + 144, at] = (sc + cs).astype(bf16)
                right[f, base + 160 : base + 176, at] = (sc - cs).astype(bf16)
        return carry

    lax.fori_loop(0, fb * n_sta - fb * n_sta // 4, table_step, 0)

    for o in range(1, n_bins):
        square_arrival(o).wait_recv()
    total = squares[0]
    for b in range(1, n_bins):
        total = total + squares[b]
    inverse = 1.0 / jnp.sqrt(total / (2 * bins_dev * n_bins) + epsilon)
    scales[me] = inverse
    for f in range(bins_dev):
        for c in range(2):
            white[c, f] = (own[c, f].astype(f32) * inverse).astype(bf16)
    if raw:

        @pl.when(sends_raw)
        def _():
            for k in range(raw):
                scale_send(k).start()

        @pl.when(jnp.logical_not(sends_raw))
        def _():
            for k in range(raw):
                await_entry(k)
                block_send(k, white).start()

    for k in range(raw, n_sta - 1):
        await_entry(k)
        block_send(k, white).start()
    for f in range(fb):
        for c in range(2):
            blocks[me, c, f] = white[c, group * fb + f]

    lax.fori_loop(fb * n_sta - fb * n_sta // 4, fb * n_sta, table_step, 0)
    product[...] = jnp.zeros_like(product)
    slow_copy.wait()
    sx = slowness[0:1, :] + 32
    sy = slowness[1:2, :] + 32
    a_index = sx // 16
    flipped = a_index < 2
    y_index = jnp.where(flipped, 63 - sy, sy)
    y_slot = jnp.where(y_index >= 32, y_index - 32, 63 - y_index)
    a_slot = jnp.where(flipped, 1 - a_index, a_index - 2)
    column = jnp.where(flipped, 128, 0) + a_slot * 64 + y_slot
    for i in range(16):
        ids = lax.broadcasted_iota(jnp.int32, (16, column.shape[1]), 0) + 16 * i
        onehot[i * 16 : (i + 1) * 16, :] = jnp.where(ids == column, 1.0, 0.0).astype(bf16)


    def turn_step(step, carry):
        at = pl.ds(pl.multiple_of(step * sta_dev, sta_dev), sta_dev)
        for f in range(fb):
            turned[f, at, :] = right[f, :, at].T
        return carry

    lax.fori_loop(0, n_sta, turn_step, 0)

    def fill(source):
        at = pl.ds(pl.multiple_of(source * sta_dev, sta_dev), sta_dev)
        for f in range(fb):
            re = blocks[source, 0, f].astype(f32)
            im = blocks[source, 1, f].astype(f32)
            c0 = rotor[f, 0, 2:3, at]
            s0 = rotor[f, 1, 2:3, at]
            parts = (re * c0 - im * s0, im * c0 + re * s0)
            trig = (cos_b[f, :, at], sin_b[f, :, at])
            for p in range(2):
                for ri in range(2):
                    for g in range(0, segs, 2):
                        both = jnp.concatenate(
                            [parts[ri][g : g + 1] * trig[p], parts[ri][g + 1 : g + 2] * trig[p]], 0
                        )
                        base = ((p * 2 + ri) * segs + g) * 8
                        left[f, base : base + 16, :] = both.astype(bf16)
            product[f] += lax.dot_general(
                left[f], turned[f, at, :], (((1,), (0,)), ((), ())), preferred_element_type=f32
            )

    def whiten(source):
        scale_arrival(source).wait_recv()
        factor = scales[source]
        for f in range(fb):
            for c in range(2):
                blocks[source, c, f] = (blocks[source, c, f].astype(f32) * factor).astype(bf16)

    def arrive_step(k, carry):
        source = origin(k)
        block_arrival(source).wait_recv()
        if raw:

            @pl.when(is_raw(source))
            def _():
                whiten(source)

        fill(source)
        return carry

    fill(me)
    lax.fori_loop(0, n_sta - 1, arrive_step, 0)

    part = segs * 8

    def bin_power(f, carry):
        sums = [None] * 4
        for g in range(segs):
            r0 = g * 8
            ccr, csr = product[f, r0 : r0 + 8, :128], product[f, r0 : r0 + 8, 128:]
            r0 += part
            cci, csi = product[f, r0 : r0 + 8, :128], product[f, r0 : r0 + 8, 128:]
            r0 += part
            scr, ssr = product[f, r0 : r0 + 8, :128], product[f, r0 : r0 + 8, 128:]
            r0 += part
            sci, ssi = product[f, r0 : r0 + 8, :128], product[f, r0 : r0 + 8, 128:]
            pr, pi, mr, mi = ccr - ssr, cci - ssi, ccr + ssr, cci + ssi
            tr, ti, dr, di = scr + csr, sci + csi, scr - csr, sci - csi
            amps = (
                (pr + ti, pi - tr),
                (mr + di, mi - dr),
                (mr - di, mi + dr),
                (pr - ti, pi + tr),
            )
            for c, (x, y) in enumerate(amps):
                power = x * x + y * y
                sums[c] = power if sums[c] is None else sums[c] + power
        grid = jnp.concatenate(
            [jnp.concatenate(sums[0:2], 1), jnp.concatenate(sums[2:4], 1)], 0
        )
        hi = grid.astype(bf16)
        lo = (grid - hi.astype(f32)).astype(bf16)
        grid_hi_lo[0, f] = hi
        grid_hi_lo[1, f] = lo
        return carry

    lax.fori_loop(0, fb, bin_power, 0)

    norm = 1.0 / (n_sta * sta_dev * segs)
    rows = jnp.concatenate(
        [grid_hi_lo[h, f] for h in range(2) for f in range(fb)], 0
    )

    def result_send(o):
        there = (group + o) % groups
        return pltpu.make_async_remote_copy(
            src_ref=picked.at[there],
            dst_ref=returned.at[group],
            send_sem=re_send.at[o],
            recv_sem=re_recv.at[group],
            device_id={"sta": there * copies + lane_of},
            device_id_type=MESH,
        )

    def result_arrival(o):
        source = (group + o) % groups
        return pltpu.make_async_remote_copy(
            src_ref=returned.at[source],
            dst_ref=returned.at[source],
            send_sem=re_send.at[o],
            recv_sem=re_recv.at[source],
            device_id={"sta": source * copies + lane_of},
            device_id_type=MESH,
        )

    ids16 = lax.broadcasted_iota(jnp.int32, (16, beams_dev), 0)
    packed_rows = 16 * fb
    for there in range(groups):
        if copies == 1:
            at = pl.ds(there * beams_dev, beams_dev)
        else:
            target = there * copies + lane_of
            at = pl.ds(pl.multiple_of(target * beams_dev, beams_dev), beams_dev)
        values = jnp.dot(rows, onehot[:, at], preferred_element_type=f32)
        values = values[:packed_rows] + values[packed_rows:]
        sx_at = slowness[0:1, at] + 32
        b_at = sx_at % 16
        row_at = jnp.where(b_at >= 8, b_at - 8, 15 - b_at)
        keep = jnp.where(ids16 == row_at, norm, 0.0)
        for f in range(fb):
            line = jnp.sum(values[f * 16 : (f + 1) * 16] * keep, axis=0, keepdims=True)
            picked[there, f : f + 1, :] = line
    for o in range(1, groups):
        result_send(o).start()
    returned[group] = picked[group]

    for o in range(1, groups):
        result_arrival(o).wait_recv()
    for g in range(groups):
        out[g * fb : (g + 1) * fb, :] = returned[g]

    for o in range(1, n_bins):
        square_send(o).wait_send()
    for k in range(n_sta - 1):
        block_send(k, white).wait_send()
    if raw:

        @pl.when(sends_raw)
        def _():
            for k in range(raw):
                scale_send(k).wait_send()

    for o in range(1, groups):
        result_send(o).wait_send()


def solution(mesh):
    n_bins, n_sta = mesh.shape["bins"], mesh.shape["sta"]

    def local(spectra, coords, slowness):
        _, bins_dev, segs, sta_dev = spectra.shape
        stations, beams = coords.shape[1], slowness.shape[1]
        beams_dev = beams // n_sta
        groups = math.gcd(bins_dev, n_sta)
        copies = n_sta // groups
        fb = bins_dev // groups
        dims = (n_bins, n_sta, groups, copies, fb, bins_dev, segs, sta_dev, beams_dev)
        f32, bf16 = jnp.float32, jnp.bfloat16
        dma = pltpu.SemaphoreType.DMA
        return pl.pallas_call(
            functools.partial(kernel, dims),
            out_shape=pltpu.VMEM((bins_dev, beams_dev), f32),
            in_specs=[
                pl.BlockSpec(memory_space=pltpu.HBM),
                pl.BlockSpec(memory_space=pltpu.HBM),
                pl.BlockSpec(memory_space=pltpu.HBM),
            ],
            out_specs=pl.BlockSpec(memory_space=pltpu.VMEM),
            scratch_shapes=[
                pltpu.VMEM((2, stations), jnp.int32),
                pltpu.VMEM((2, beams), jnp.int32),
                pltpu.VMEM((2, bins_dev, segs, sta_dev), bf16),
                pltpu.VMEM((2, bins_dev, segs, sta_dev), bf16),
                pltpu.VMEM((n_sta, 2, fb, segs, sta_dev), bf16),
                pltpu.VMEM((n_bins, segs, sta_dev), f32),
                pltpu.VMEM((n_sta, segs, sta_dev), f32),
                pltpu.VMEM((fb, 8, stations), f32),
                pltpu.VMEM((fb, 8, stations), f32),
                pltpu.VMEM((fb, 2, 8, stations), f32),
                pltpu.VMEM((fb, 256, stations), bf16),
                pltpu.VMEM((fb, stations, 256), bf16),
                pltpu.VMEM((fb, 32 * segs, sta_dev), bf16),
                pltpu.VMEM((fb, 32 * segs, 256), f32),
                pltpu.VMEM((2, fb, 16, 256), bf16),
                pltpu.VMEM((256, beams), bf16),
                pltpu.VMEM((n_sta, fb, beams_dev), f32),
                pltpu.VMEM((groups, fb, beams_dev), f32),
                pltpu.SemaphoreType.REGULAR((n_sta,)),
                dma,
                dma,
                dma,
                dma((n_bins,)),
                dma((n_bins,)),
                dma((max(2, n_sta),)),
                dma((n_sta,)),
                dma((n_sta,)),
                dma((n_sta,)),
                dma((groups,)),
                dma((groups,)),
            ],
            compiler_params=pltpu.CompilerParams(
                collective_id=0,
                has_side_effects=True,
                vmem_limit_bytes=33554432,
            ),
            name="beam_power",
        )(*(pltpu.with_memory_space_constraint(x, pltpu.HBM) for x in (spectra, coords, slowness)))

    in_specs = (P(None, "bins", None, "sta"), P(), P())
    out_specs = P("bins", "sta")
    return jax.shard_map(local, mesh=mesh, in_specs=in_specs, out_specs=out_specs, check_vma=False)
```

```python
import functools
import math

import jax
import jax.numpy as jnp
from jax import lax
from jax.experimental import pallas as pl
from jax.experimental.pallas import tpu as pltpu
from jax.sharding import PartitionSpec as P

epsilon = 1e-06
MESH = pl.DeviceIdType.MESH

SIN_COEFS = (6.28318501, -41.3415909, 81.5999451, -76.6144714, 41.3428841, -12.4712439)
COS_COEFS = (1.0, -19.7392044, 64.9391174, -85.4501419, 60.1676292, -25.9675999, 6.52865839)


def horner(coefs, z):
    acc = jnp.full_like(z, coefs[-1])
    for c in coefs[-2::-1]:
        acc = acc * z + c
    return acc


def cos_sin(index):
    turns = (index << 11).astype(jnp.float32) * (2.0 ** -32)
    z = turns * turns
    return horner(COS_COEFS, z), horner(SIN_COEFS, z) * turns


def kernel(
    dims,
    spectra,
    coords_hbm,
    slowness_hbm,
    out,
    coords,
    slowness,
    own,
    white,
    blocks,
    squares,
    scales,
    cos_b,
    sin_b,
    rotor,
    right,
    turned,
    left,
    product,
    grid_hi_lo,
    onehot,
    keep,
    picked,
    returned,
    entered,
    own_sem,
    coords_sem,
    slow_sem,
    sq_send,
    sq_recv,
    sc_send,
    sc_recv,
    bl_send,
    bl_recv,
    re_send,
    re_recv,
):
    n_bins, n_sta, groups, copies, fb, extra, bins_dev, segs, sta_dev, beams_dev = dims
    me = lax.axis_index("sta")
    mb = lax.axis_index("bins")
    group = me // copies
    lane_of = me % copies
    f32, bf16 = jnp.float32, jnp.bfloat16
    most = fb + extra

    paired = n_sta >= 4 and n_sta & (n_sta - 1) == 0
    half = n_sta // 2
    upper = me // half if paired else 0

    edge = n_sta // 4
    raw = 2 if paired else 0

    def partner(k):
        if not paired:
            return (me + k + 1) % n_sta
        flip = me & 1
        if k < 2:
            early = half - 2 + k
        elif k < half:
            early = me ^ k ^ flip
        elif k < n_sta - 2:
            early = k - half
        else:
            early = me ^ 1 ^ flip
        if k < half:
            late = half + k if half < 4 else ((half, n_sta - 2, n_sta - 1)[k] if k < 3 else half + k - 2)
        else:
            late = me ^ (k - half + 2 if k < n_sta - 2 else 1) ^ flip
        return jnp.where(upper == 1, early, late) ^ flip

    def origin(k):
        if not paired:
            return (me - k - 1 + n_sta) % n_sta
        inner = jnp.logical_and(me >= edge, me < half)
        far = jnp.where(inner, k - 1, k - (half - 1))
        aside = jnp.where(jnp.logical_and(inner, k > 0), k - half + 1, k + 1)
        other = jnp.where(upper == 1, far, jnp.where(me < edge, n_sta - 1 - far, half + far))
        return jnp.where(jnp.logical_and(far >= 0, far < half), other, me ^ aside)

    def first_of(part):
        if extra:
            return part * most - jnp.maximum(part - half, 0) * extra
        return part * fb

    def is_long(part):
        return part < half

    long_me = is_long(group)
    bins_me = jnp.where(long_me, most, fb)
    first_me = first_of(group)
    sends_raw = upper == 1
    prompt = mb % 2 == 0

    def is_raw(source):
        return jnp.logical_and(
            source // half == 1, jnp.logical_and(me >= half - 2, me < half)
        )

    own_copy = pltpu.make_async_copy(spectra, own, own_sem)
    own_copy.start()
    coords_copy = pltpu.make_async_copy(coords_hbm, coords, coords_sem)
    coords_copy.start()
    slow_copy = pltpu.make_async_copy(slowness_hbm, slowness, slow_sem)
    slow_copy.start()

    barrier = pltpu.get_barrier_semaphore()
    for o in range(1, n_bins):
        pl.semaphore_signal(
            barrier, inc=1, device_id={"bins": (mb + o) % n_bins}, device_id_type=MESH
        )
    for o in range(1, n_sta):
        later = me + o

        @pl.when(later < n_sta)
        def _():
            pl.semaphore_signal(
                barrier, inc=1, device_id={"sta": later}, device_id_type=MESH
            )

    own_copy.wait()

    def square_step(f, acc):
        re = own[0, f].astype(f32)
        im = own[1, f].astype(f32)
        return acc + re * re + im * im

    squares[mb] = lax.fori_loop(
        0, bins_dev, square_step, jnp.zeros((segs, sta_dev), f32), unroll=True
    )

    pl.semaphore_wait(barrier, n_bins - 1 + me)
    for o in range(1, n_sta):
        earlier = me - o

        @pl.when(earlier >= 0)
        def _():
            pl.semaphore_signal(
                entered.at[me], inc=1, device_id={"sta": earlier}, device_id_type=MESH
            )


    def square_send(o):
        return pltpu.make_async_remote_copy(
            src_ref=squares.at[mb],
            dst_ref=squares.at[mb],
            send_sem=sq_send,
            recv_sem=sq_recv,
            device_id={"bins": (mb + o) % n_bins},
            device_id_type=MESH,
        )

    def squares_of(count):
        return pltpu.make_async_remote_copy(
            src_ref=squares.at[pl.ds(0, count)],
            dst_ref=squares.at[pl.ds(0, count)],
            send_sem=sq_send,
            recv_sem=sq_recv,
            device_id={"bins": mb},
            device_id_type=MESH,
        )

    def scale_send(k):
        return pltpu.make_async_remote_copy(
            src_ref=scales.at[me],
            dst_ref=scales.at[me],
            send_sem=sc_send,
            recv_sem=sc_recv.at[me - half],
            device_id={"sta": partner(k)},
            device_id_type=MESH,
        )

    def scale_arrival(source):
        return pltpu.make_async_remote_copy(
            src_ref=scales.at[source],
            dst_ref=scales.at[source],
            send_sem=sc_send,
            recv_sem=sc_recv.at[source - half],
            device_id={"sta": source},
            device_id_type=MESH,
        )

    def block_copy(k, values, begin, count):
        target = partner(k)
        return pltpu.make_async_remote_copy(
            src_ref=values.at[:, pl.ds(first_of(target // copies) + begin, count)],
            dst_ref=blocks.at[me, :, pl.ds(begin, count)],
            send_sem=bl_send,
            recv_sem=bl_recv.at[me],
            device_id={"sta": target},
            device_id_type=MESH,
        )

    def block_send(k, values):
        block_copy(k, values, 0, fb).start()
        if extra:

            @pl.when(is_long(partner(k)))
            def _():
                block_copy(k, values, fb, extra).start()

    def blocks_sent():
        def wait(ref):
            pltpu.make_async_remote_copy(
                src_ref=ref,
                dst_ref=ref,
                send_sem=bl_send,
                recv_sem=bl_recv.at[me],
                device_id={"sta": me},
                device_id_type=MESH,
            ).wait_send()

        if not extra:
            wait(blocks.at[pl.ds(0, n_sta - 1)])
            return

        @pl.when(long_me)
        def _():
            wait(white.at[:, pl.ds(0, bins_dev - most)])

        @pl.when(jnp.logical_not(long_me))
        def _():
            wait(white.at[:, pl.ds(0, bins_dev - fb)])

    def scales_of(count):
        return pltpu.make_async_remote_copy(
            src_ref=scales.at[pl.ds(0, count)],
            dst_ref=scales.at[pl.ds(0, count)],
            send_sem=sc_send,
            recv_sem=sc_recv.at[0],
            device_id={"sta": me},
            device_id_type=MESH,
        )

    def await_entry(k):
        target = partner(k)

        @pl.when(target > me)
        def _():
            pl.semaphore_wait(entered.at[target], 1)

    def block_arrival(source, count):
        return pltpu.make_async_remote_copy(
            src_ref=blocks.at[source, :, pl.ds(0, count)],
            dst_ref=blocks.at[source, :, pl.ds(0, count)],
            send_sem=bl_send,
            recv_sem=bl_recv.at[source],
            device_id={"sta": source},
            device_id_type=MESH,
        )

    for o in range(1, n_bins):
        square_send(o).start()
    if raw:

        @pl.when(sends_raw)
        def _():
            for k in range(raw):
                await_entry(k)
                block_send(k, own)


    coords_copy.wait()
    first_bin = mb * bins_dev + first_me + 1

    def table_step(step, carry):
        f = step // n_sta
        at = pl.ds(pl.multiple_of((step % n_sta) * sta_dev, sta_dev), sta_dev)
        bin_number = first_bin + f
        east = coords[0:1, at] * bin_number
        north = coords[1:2, at] * bin_number
        ids = lax.broadcasted_iota(jnp.int32, (8, sta_dev), 0)
        cb, sb = cos_sin((2 * ids + 1) * east)
        cos_b[f, :, at] = cb
        sin_b[f, :, at] = sb
        steps = jnp.where(ids == 0, 16, jnp.where(ids == 1, 48, 1))
        ca, sa = cos_sin(steps * east + jnp.where(ids == 2, north, 0))
        rotor[f, 0, :, at] = ca
        rotor[f, 1, :, at] = sa
        ids = lax.broadcasted_iota(jnp.int32, (16, sta_dev), 0)
        for half in range(2):
            cy, sy = cos_sin((2 * ids + (32 * half + 1)) * north)
            for a in range(2):
                c, s = ca[a : a + 1], sa[a : a + 1]
                cc, ss, sc, cs = c * cy, s * sy, s * cy, c * sy
                base = a * 64 + half * 16
                right[f, base : base + 16, at] = (cc - ss).astype(bf16)
                right[f, base + 32 : base + 48, at] = (cc + ss).astype(bf16)
                right[f, base + 128 : base + 144, at] = (sc + cs).astype(bf16)
                right[f, base + 160 : base + 176, at] = (sc - cs).astype(bf16)
        return carry

    lax.fori_loop(0, fb * n_sta, table_step, 0)

    if n_bins > 1:
        squares_of(n_bins - 1).wait_recv()
    total = squares[0]
    for b in range(1, n_bins):
        total = total + squares[b]
    inverse = 1.0 / jnp.sqrt(total / (2 * bins_dev * n_bins) + epsilon)
    scales[me] = inverse
    for f in range(bins_dev):
        for c in range(2):
            white[c, f] = (own[c, f].astype(f32) * inverse).astype(bf16)
    if raw:

        @pl.when(sends_raw)
        def _():
            for k in range(raw):
                scale_send(k).start()

    def crosses(k):
        late_far = 1 if k < half else 0
        early_far = 1 if half <= k < n_sta - 2 else 0
        return jnp.where(upper == 1, early_far, late_far) == 1

    def white_send(k, wanted):
        if k < raw:
            wanted = jnp.logical_and(wanted, jnp.logical_not(sends_raw))

        @pl.when(wanted)
        def _():
            await_entry(k)
            block_send(k, white)

    for k in range(n_sta - 1):
        if paired:
            white_send(k, jnp.logical_or(prompt, jnp.logical_not(crosses(k))))
        else:
            white_send(k, True)

    for f in range(fb):
        for c in range(2):
            blocks[me, c, f] = white[c, first_me + f]
    if extra:

        @pl.when(long_me)
        def _():
            for f in range(fb, most):
                for c in range(2):
                    blocks[me, c, f] = white[c, first_me + f]

    if extra:
        lax.fori_loop(fb * n_sta, bins_me * n_sta, table_step, 0)
    product[...] = jnp.zeros_like(product)
    slow_copy.wait()
    sx = slowness[0:1, :] + 32
    sy = slowness[1:2, :] + 32
    a_index = sx // 16
    flipped = a_index < 2
    y_index = jnp.where(flipped, 63 - sy, sy)
    y_slot = jnp.where(y_index >= 32, y_index - 32, 63 - y_index)
    a_slot = jnp.where(flipped, 1 - a_index, a_index - 2)
    column = jnp.where(flipped, 128, 0) + a_slot * 64 + y_slot
    for i in range(16):
        ids = lax.broadcasted_iota(jnp.int32, (16, column.shape[1]), 0) + 16 * i
        onehot[i * 16 : (i + 1) * 16, :] = jnp.where(ids == column, 1.0, 0.0).astype(bf16)
    norm = 1.0 / (n_sta * sta_dev * segs)
    b_index = sx % 16
    row = jnp.where(b_index >= 8, b_index - 8, 15 - b_index)
    ids = lax.broadcasted_iota(jnp.int32, (16, column.shape[1]), 0)
    keep[...] = jnp.where(ids == row, norm, 0.0)


    def turn(begin, end):
        def turn_step(step, carry):
            at = pl.ds(pl.multiple_of(step * sta_dev, sta_dev), sta_dev)
            for f in range(begin, end):
                turned[f, at, :] = right[f, :, at].T
            return carry

        lax.fori_loop(0, n_sta, turn_step, 0)

    def late_sends(when):
        for k in range(n_sta - 2):
            white_send(k, jnp.logical_and(jnp.logical_and(jnp.logical_not(prompt), when), crosses(k)))

    if paired:
        late_sends(upper == 0)
    turn(0, fb)
    if paired:
        late_sends(upper == 1)
    if extra:

        @pl.when(long_me)
        def _():
            turn(fb, most)

    def fill(source, count):
        at = pl.ds(pl.multiple_of(source * sta_dev, sta_dev), sta_dev)
        for f in range(count):
            re = blocks[source, 0, f].astype(f32)
            im = blocks[source, 1, f].astype(f32)
            c0 = rotor[f, 0, 2:3, at]
            s0 = rotor[f, 1, 2:3, at]
            parts = (re * c0 - im * s0, im * c0 + re * s0)
            trig = (cos_b[f, :, at], sin_b[f, :, at])
            for p in range(2):
                for ri in range(2):
                    for g in range(0, segs, 2):
                        both = jnp.concatenate(
                            [parts[ri][g : g + 1] * trig[p], parts[ri][g + 1 : g + 2] * trig[p]], 0
                        )
                        base = ((p * 2 + ri) * segs + g) * 8
                        left[f, base : base + 16, :] = both.astype(bf16)
            product[f] += lax.dot_general(
                left[f], turned[f, at, :], (((1,), (0,)), ((), ())), preferred_element_type=f32
            )

    def whiten(source, count):
        scale_arrival(source).wait_recv()
        factor = scales[source]
        for f in range(count):
            for c in range(2):
                blocks[source, c, f] = (blocks[source, c, f].astype(f32) * factor).astype(bf16)

    def take(k, count, may_be_raw):
        source = jnp.where(k == 0, me, origin(k - 1))

        @pl.when(k > 0)
        def _():
            block_arrival(source, count).wait_recv()

        if may_be_raw:

            @pl.when(jnp.logical_and(k > 0, is_raw(source)))
            def _():
                whiten(source, count)

        fill(source, count)

    def arrive_step(k, carry):
        if not extra:
            take(k, fb, raw > 0)
            return carry

        @pl.when(long_me)
        def _():
            take(k, most, True)

        @pl.when(jnp.logical_not(long_me))
        def _():
            take(k, fb, False)

        return carry

    lax.fori_loop(0, n_sta, arrive_step, 0)

    part = segs * 8

    def bin_power(f, carry):
        sums = [None] * 4
        for g in range(segs):
            r0 = g * 8
            ccr, csr = product[f, r0 : r0 + 8, :128], product[f, r0 : r0 + 8, 128:]
            r0 += part
            cci, csi = product[f, r0 : r0 + 8, :128], product[f, r0 : r0 + 8, 128:]
            r0 += part
            scr, ssr = product[f, r0 : r0 + 8, :128], product[f, r0 : r0 + 8, 128:]
            r0 += part
            sci, ssi = product[f, r0 : r0 + 8, :128], product[f, r0 : r0 + 8, 128:]
            pr, pi, mr, mi = ccr - ssr, cci - ssi, ccr + ssr, cci + ssi
            tr, ti, dr, di = scr + csr, sci + csi, scr - csr, sci - csi
            amps = (
                (pr + ti, pi - tr),
                (mr + di, mi - dr),
                (mr - di, mi + dr),
                (pr - ti, pi + tr),
            )
            for c, (x, y) in enumerate(amps):
                power = x * x + y * y
                sums[c] = power if sums[c] is None else sums[c] + power
        grid = jnp.concatenate(
            [jnp.concatenate(sums[0:2], 1), jnp.concatenate(sums[2:4], 1)], 0
        )
        hi = grid.astype(bf16)
        lo = (grid - hi.astype(f32)).astype(bf16)
        grid_hi_lo[0, f] = hi
        grid_hi_lo[1, f] = lo
        return carry

    lax.fori_loop(0, most, bin_power, 0)

    rows = jnp.concatenate(
        [grid_hi_lo[h, f] for h in range(2) for f in range(most)], 0
    )

    def result_send(there):
        return pltpu.make_async_remote_copy(
            src_ref=picked.at[there],
            dst_ref=returned.at[group],
            send_sem=re_send,
            recv_sem=re_recv,
            device_id={"sta": there * copies + lane_of},
            device_id_type=MESH,
        )

    def results_of(count):
        return pltpu.make_async_remote_copy(
            src_ref=returned.at[pl.ds(0, count)],
            dst_ref=returned.at[pl.ds(0, count)],
            send_sem=re_send,
            recv_sem=re_recv,
            device_id={"sta": me},
            device_id_type=MESH,
        )

    packed_rows = 16 * most
    def pick(there):
        if copies == 1:
            at = pl.ds(there * beams_dev, beams_dev)
        else:
            target = there * copies + lane_of
            at = pl.ds(pl.multiple_of(target * beams_dev, beams_dev), beams_dev)
        values = jnp.dot(rows, onehot[:, at], preferred_element_type=f32)
        values = values[:packed_rows] + values[packed_rows:]
        for f in range(most):
            line = jnp.sum(values[f * 16 : (f + 1) * 16] * keep[:, at], axis=0, keepdims=True)
            picked[there, f : f + 1, :] = line

    soon = min(2, groups)
    for span in (range(soon), range(soon, groups)):
        for there in span:
            pick(there)
        for there in span:

            @pl.when(there != group)
            def _():
                result_send(there).start()

    returned[group] = picked[group]

    if groups > 1:
        results_of(groups - 1).wait_recv()
    for g in range(groups):
        count = most if not extra or g < half else fb
        begin = g * most - max(g - half, 0) * extra
        out[begin : begin + count, :] = returned[g, :count]

    if n_bins > 1:
        squares_of(n_bins - 1).wait_send()
    if n_sta > 1:
        blocks_sent()
    if raw:

        @pl.when(sends_raw)
        def _():
            scales_of(raw).wait_send()

    if groups > 1:
        results_of(groups - 1).wait_send()


def solution(mesh):
    n_bins, n_sta = mesh.shape["bins"], mesh.shape["sta"]

    def local(spectra, coords, slowness):
        _, bins_dev, segs, sta_dev = spectra.shape
        stations, beams = coords.shape[1], slowness.shape[1]
        beams_dev = beams // n_sta
        groups = math.gcd(bins_dev, n_sta)
        copies = n_sta // groups
        fb = bins_dev // groups
        extra = 0
        if copies == 1 and n_sta >= 4 and n_sta & (n_sta - 1) == 0 and fb >= 4:
            extra = 2 * (fb // 4)
            fb = fb - fb // 4
        most = fb + extra
        dims = (n_bins, n_sta, groups, copies, fb, extra, bins_dev, segs, sta_dev, beams_dev)
        f32, bf16 = jnp.float32, jnp.bfloat16
        dma = pltpu.SemaphoreType.DMA
        return pl.pallas_call(
            functools.partial(kernel, dims),
            out_shape=pltpu.VMEM((bins_dev, beams_dev), f32),
            in_specs=[
                pl.BlockSpec(memory_space=pltpu.HBM),
                pl.BlockSpec(memory_space=pltpu.HBM),
                pl.BlockSpec(memory_space=pltpu.HBM),
            ],
            out_specs=pl.BlockSpec(memory_space=pltpu.VMEM),
            scratch_shapes=[
                pltpu.VMEM((2, stations), jnp.int32),
                pltpu.VMEM((2, beams), jnp.int32),
                pltpu.VMEM((2, bins_dev, segs, sta_dev), bf16),
                pltpu.VMEM((2, bins_dev, segs, sta_dev), bf16),
                pltpu.VMEM((n_sta, 2, most, segs, sta_dev), bf16),
                pltpu.VMEM((n_bins, segs, sta_dev), f32),
                pltpu.VMEM((n_sta, segs, sta_dev), f32),
                pltpu.VMEM((most, 8, stations), f32),
                pltpu.VMEM((most, 8, stations), f32),
                pltpu.VMEM((most, 2, 8, stations), f32),
                pltpu.VMEM((most, 256, stations), bf16),
                pltpu.VMEM((most, stations, 256), bf16),
                pltpu.VMEM((most, 32 * segs, sta_dev), bf16),
                pltpu.VMEM((most, 32 * segs, 256), f32),
                pltpu.VMEM((2, most, 16, 256), bf16),
                pltpu.VMEM((256, beams), bf16),
                pltpu.VMEM((16, beams), f32),
                pltpu.VMEM((n_sta, most, beams_dev), f32),
                pltpu.VMEM((groups, most, beams_dev), f32),
                pltpu.SemaphoreType.REGULAR((n_sta,)),
                dma,
                dma,
                dma,
                dma,
                dma,
                dma,
                dma((max(1, n_sta // 2),)),
                dma,
                dma((n_sta,)),
                dma,
                dma,
            ],
            compiler_params=pltpu.CompilerParams(
                collective_id=0,
                has_side_effects=True,
                vmem_limit_bytes=33554432,
            ),
            name="beam_power",
        )(*(pltpu.with_memory_space_constraint(x, pltpu.HBM) for x in (spectra, coords, slowness)))

    in_specs = (P(None, "bins", None, "sta"), P(), P())
    out_specs = P("bins", "sta")
    return jax.shard_map(local, mesh=mesh, in_specs=in_specs, out_specs=out_specs, check_vma=False)
```

```python
import functools
import math

import jax
import jax.numpy as jnp
from jax import lax
from jax.experimental import pallas as pl
from jax.experimental.pallas import tpu as pltpu
from jax.sharding import PartitionSpec as P

epsilon = 1e-06
MESH = pl.DeviceIdType.MESH

SIN_COEFS = (6.28318501, -41.3415909, 81.5999451, -76.6144714, 41.3428841, -12.4712439)
COS_COEFS = (1.0, -19.7392044, 64.9391174, -85.4501419, 60.1676292, -25.9675999, 6.52865839)


def horner(coefs, z):
    acc = jnp.full_like(z, coefs[-1])
    for c in coefs[-2::-1]:
        acc = acc * z + c
    return acc


def cos_sin(index):
    turns = (index << 11).astype(jnp.float32) * (2.0 ** -32)
    z = turns * turns
    return horner(COS_COEFS, z), horner(SIN_COEFS, z) * turns


def kernel(
    dims,
    spectra,
    coords_hbm,
    slowness_hbm,
    out,
    coords,
    slowness,
    own,
    white,
    blocks,
    squares,
    scales,
    cos_b,
    sin_b,
    rotor,
    right,
    turned,
    left,
    product,
    grid_hi_lo,
    onehot,
    keep,
    picked,
    returned,
    entered,
    own_sem,
    coords_sem,
    slow_sem,
    sq_send,
    sq_recv,
    sc_send,
    sc_recv,
    bl_send,
    bl_recv,
    re_send,
    re_recv,
):
    n_bins, n_sta, groups, copies, fb, extra, bins_dev, segs, sta_dev, beams_dev = dims
    me = lax.axis_index("sta")
    mb = lax.axis_index("bins")
    group = me // copies
    lane_of = me % copies
    f32, bf16 = jnp.float32, jnp.bfloat16
    most = fb + extra

    paired = n_sta >= 4 and n_sta & (n_sta - 1) == 0
    half = n_sta // 2
    upper = me // half if paired else 0

    edge = n_sta // 4
    raw = 2 if paired else 0

    def partner(k):
        if not paired:
            return (me + k + 1) % n_sta
        flip = me & 1
        if k < 2:
            early = half - 2 + k
        elif k < half:
            early = me ^ k ^ flip
        elif k < n_sta - 2:
            early = k - half
        else:
            early = me ^ 1 ^ flip
        if k < half:
            late = half + k if half < 4 else ((half, n_sta - 2, n_sta - 1)[k] if k < 3 else half + k - 2)
            across = me + edge
            rest = n_sta - k
            rest = across if k == 0 else rest - jnp.where(rest <= across, 1, 0)
            if k in (1, 2) and half >= 4:
                rest = rest ^ (1 - flip)
            late = jnp.where(me < edge, late, rest ^ flip)
        else:
            late = me ^ (k - half + 2 if k < n_sta - 2 else 1) ^ flip
        return jnp.where(upper == 1, early, late) ^ flip

    def origin(k):
        if not paired:
            return (me - k - 1 + n_sta) % n_sta
        outer = k - (half - 1)
        spread = half + outer
        if half >= 4:
            spread = jnp.where(outer == 0, half, n_sta - 3 + outer)
            spread = jnp.where(outer > 2, half + outer - 2, spread)
        at_edge = jnp.where(outer < 0, me ^ (k + 1), spread ^ (me & 1))
        at_inner = jnp.where(k < half, half + k, me ^ (k - half + 1))
        side = me & 1
        at_upper = jnp.where(k == 0, me ^ 1, k - 1)
        if half >= 4:
            cross = 2 * (n_sta - 2 - k) + 1 - side
            at_upper = jnp.where(k < half + half // 2 - 1, me ^ (k - half // 2 + 1), cross)
            at_upper = jnp.where(k < half // 2 + 2, 2 * (k - 2) + side, at_upper)
            at_upper = jnp.where(k < 2, me ^ (k + 1), at_upper)
        return jnp.where(upper == 1, at_upper, jnp.where(me < edge, at_edge, at_inner))

    def first_of(part):
        if extra:
            return part * most - jnp.maximum(part - half, 0) * extra
        return part * fb

    def is_long(part):
        return part < half

    long_me = is_long(group)
    bins_me = jnp.where(long_me, most, fb)
    first_me = first_of(group)
    prompt = mb % 2 == 0

    inner = jnp.logical_and(me >= edge, me < half)

    def sent_raw(k):
        if not raw or k >= raw:
            return False
        return jnp.logical_or(upper == 1, inner) if k == 0 else upper == 1

    def is_raw(source):
        from_far = jnp.logical_and(
            source // half == 1, jnp.logical_and(me >= half - 2, me < half)
        )
        from_near = jnp.logical_and(
            source == me - edge, jnp.logical_and(me >= half, me < half + edge)
        )
        return jnp.logical_or(from_far, from_near)

    def scale_slot(source):
        return jnp.maximum(source - half, 0)

    own_copy = pltpu.make_async_copy(spectra, own, own_sem)
    own_copy.start()
    coords_copy = pltpu.make_async_copy(coords_hbm, coords, coords_sem)
    coords_copy.start()
    slow_copy = pltpu.make_async_copy(slowness_hbm, slowness, slow_sem)
    slow_copy.start()

    barrier = pltpu.get_barrier_semaphore()
    for o in range(1, n_bins):
        pl.semaphore_signal(
            barrier, inc=1, device_id={"bins": (mb + o) % n_bins}, device_id_type=MESH
        )
    for o in range(1, n_sta):
        later = me + o

        @pl.when(later < n_sta)
        def _():
            pl.semaphore_signal(
                barrier, inc=1, device_id={"sta": later}, device_id_type=MESH
            )

    own_copy.wait()

    def square_step(f, acc):
        re = own[0, f].astype(f32)
        im = own[1, f].astype(f32)
        return acc + re * re + im * im

    squares[mb] = lax.fori_loop(
        0, bins_dev, square_step, jnp.zeros((segs, sta_dev), f32), unroll=True
    )

    pl.semaphore_wait(barrier, n_bins - 1 + me)
    for o in range(1, n_sta):
        earlier = me - o

        @pl.when(earlier >= 0)
        def _():
            pl.semaphore_signal(
                entered.at[me], inc=1, device_id={"sta": earlier}, device_id_type=MESH
            )


    def square_send(o):
        return pltpu.make_async_remote_copy(
            src_ref=squares.at[mb],
            dst_ref=squares.at[mb],
            send_sem=sq_send,
            recv_sem=sq_recv,
            device_id={"bins": (mb + o) % n_bins},
            device_id_type=MESH,
        )

    def squares_of(count):
        return pltpu.make_async_remote_copy(
            src_ref=squares.at[pl.ds(0, count)],
            dst_ref=squares.at[pl.ds(0, count)],
            send_sem=sq_send,
            recv_sem=sq_recv,
            device_id={"bins": mb},
            device_id_type=MESH,
        )

    def scale_send(k):
        return pltpu.make_async_remote_copy(
            src_ref=scales.at[me],
            dst_ref=scales.at[me],
            send_sem=sc_send,
            recv_sem=sc_recv.at[scale_slot(me)],
            device_id={"sta": partner(k)},
            device_id_type=MESH,
        )

    def scale_arrival(source):
        return pltpu.make_async_remote_copy(
            src_ref=scales.at[source],
            dst_ref=scales.at[source],
            send_sem=sc_send,
            recv_sem=sc_recv.at[scale_slot(source)],
            device_id={"sta": source},
            device_id_type=MESH,
        )

    def block_copy(k, values, begin, count):
        target = partner(k)
        return pltpu.make_async_remote_copy(
            src_ref=values.at[:, pl.ds(first_of(target // copies) + begin, count)],
            dst_ref=blocks.at[me, :, pl.ds(begin, count)],
            send_sem=bl_send,
            recv_sem=bl_recv.at[me],
            device_id={"sta": target},
            device_id_type=MESH,
        )

    def block_send(k, values):
        block_copy(k, values, 0, fb).start()
        if extra:

            @pl.when(is_long(partner(k)))
            def _():
                block_copy(k, values, fb, extra).start()

    def blocks_sent():
        def wait(ref):
            pltpu.make_async_remote_copy(
                src_ref=ref,
                dst_ref=ref,
                send_sem=bl_send,
                recv_sem=bl_recv.at[me],
                device_id={"sta": me},
                device_id_type=MESH,
            ).wait_send()

        if not extra:
            wait(blocks.at[pl.ds(0, n_sta - 1)])
            return

        @pl.when(long_me)
        def _():
            wait(white.at[:, pl.ds(0, bins_dev - most)])

        @pl.when(jnp.logical_not(long_me))
        def _():
            wait(white.at[:, pl.ds(0, bins_dev - fb)])

    def scales_of(count):
        return pltpu.make_async_remote_copy(
            src_ref=scales.at[pl.ds(0, count)],
            dst_ref=scales.at[pl.ds(0, count)],
            send_sem=sc_send,
            recv_sem=sc_recv.at[0],
            device_id={"sta": me},
            device_id_type=MESH,
        )

    def await_entry(k):
        target = partner(k)

        @pl.when(target > me)
        def _():
            pl.semaphore_wait(entered.at[target], 1)

    def block_arrival(source, count):
        return pltpu.make_async_remote_copy(
            src_ref=blocks.at[source, :, pl.ds(0, count)],
            dst_ref=blocks.at[source, :, pl.ds(0, count)],
            send_sem=bl_send,
            recv_sem=bl_recv.at[source],
            device_id={"sta": source},
            device_id_type=MESH,
        )

    for o in range(1, n_bins):
        square_send(o).start()
    def raw_sends(when):
        for k in range(raw):

            @pl.when(jnp.logical_and(sent_raw(k), when))
            def _():
                await_entry(k)
                block_send(k, own)

    raw_sends(upper == 1)

    coords_copy.wait()
    first_bin = mb * bins_dev + first_me + 1

    def table_step(step, carry):
        f = step // n_sta
        at = pl.ds(pl.multiple_of((step % n_sta) * sta_dev, sta_dev), sta_dev)
        bin_number = first_bin + f
        east = coords[0:1, at] * bin_number
        north = coords[1:2, at] * bin_number
        ids = lax.broadcasted_iota(jnp.int32, (8, sta_dev), 0)
        cb, sb = cos_sin((2 * ids + 1) * east)
        cos_b[f, :, at] = cb
        sin_b[f, :, at] = sb
        steps = jnp.where(ids == 0, 16, jnp.where(ids == 1, 48, 1))
        ca, sa = cos_sin(steps * east + jnp.where(ids == 2, north, 0))
        rotor[f, 0, :, at] = ca
        rotor[f, 1, :, at] = sa
        ids = lax.broadcasted_iota(jnp.int32, (16, sta_dev), 0)
        for half in range(2):
            cy, sy = cos_sin((2 * ids + (32 * half + 1)) * north)
            for a in range(2):
                c, s = ca[a : a + 1], sa[a : a + 1]
                cc, ss, sc, cs = c * cy, s * sy, s * cy, c * sy
                base = a * 64 + half * 16
                right[f, base : base + 16, at] = (cc - ss).astype(bf16)
                right[f, base + 32 : base + 48, at] = (cc + ss).astype(bf16)
                right[f, base + 128 : base + 144, at] = (sc + cs).astype(bf16)
                right[f, base + 160 : base + 176, at] = (sc - cs).astype(bf16)
        return carry

    most_steps = fb * n_sta - fb * n_sta // 4
    lax.fori_loop(0, most_steps, table_step, 0)
    raw_sends(inner)
    lax.fori_loop(most_steps, fb * n_sta, table_step, 0)

    if n_bins > 1:
        squares_of(n_bins - 1).wait_recv()
    total = squares[0]
    for b in range(1, n_bins):
        total = total + squares[b]
    inverse = 1.0 / jnp.sqrt(total / (2 * bins_dev * n_bins) + epsilon)
    scales[me] = inverse
    for f in range(bins_dev):
        for c in range(2):
            white[c, f] = (own[c, f].astype(f32) * inverse).astype(bf16)
    for k in range(raw):

        @pl.when(sent_raw(k))
        def _():
            scale_send(k).start()

    def crosses(k):
        late_far = 1 if k < half else 0
        early_far = 1 if half <= k < n_sta - 2 else 0
        return jnp.where(upper == 1, early_far, late_far) == 1

    def white_send(k, wanted):
        if k < raw:
            wanted = jnp.logical_and(wanted, jnp.logical_not(sent_raw(k)))

        @pl.when(wanted)
        def _():
            await_entry(k)
            block_send(k, white)

    for k in range(n_sta - 1):
        if paired:
            white_send(k, jnp.logical_or(prompt, jnp.logical_not(crosses(k))))
        else:
            white_send(k, True)

    for f in range(fb):
        for c in range(2):
            blocks[me, c, f] = white[c, first_me + f]
    if extra:

        @pl.when(long_me)
        def _():
            for f in range(fb, most):
                for c in range(2):
                    blocks[me, c, f] = white[c, first_me + f]

    if extra:
        lax.fori_loop(fb * n_sta, bins_me * n_sta, table_step, 0)
    product[...] = jnp.zeros_like(product)
    slow_copy.wait()
    sx = slowness[0:1, :] + 32
    sy = slowness[1:2, :] + 32
    a_index = sx // 16
    flipped = a_index < 2
    y_index = jnp.where(flipped, 63 - sy, sy)
    y_slot = jnp.where(y_index >= 32, y_index - 32, 63 - y_index)
    a_slot = jnp.where(flipped, 1 - a_index, a_index - 2)
    column = jnp.where(flipped, 128, 0) + a_slot * 64 + y_slot
    for i in range(16):
        ids = lax.broadcasted_iota(jnp.int32, (16, column.shape[1]), 0) + 16 * i
        onehot[i * 16 : (i + 1) * 16, :] = jnp.where(ids == column, 1.0, 0.0).astype(bf16)
    norm = 1.0 / (n_sta * sta_dev * segs)
    b_index = sx % 16
    row = jnp.where(b_index >= 8, b_index - 8, 15 - b_index)
    ids = lax.broadcasted_iota(jnp.int32, (16, column.shape[1]), 0)
    keep[...] = jnp.where(ids == row, norm, 0.0)


    def turn(begin, end):
        def turn_step(step, carry):
            at = pl.ds(pl.multiple_of(step * sta_dev, sta_dev), sta_dev)
            for f in range(begin, end):
                turned[f, at, :] = right[f, :, at].T
            return carry

        lax.fori_loop(0, n_sta, turn_step, 0)

    def late_sends(when):
        for k in range(n_sta - 2):
            white_send(k, jnp.logical_and(jnp.logical_and(jnp.logical_not(prompt), when), crosses(k)))

    if paired:
        late_sends(upper == 0)
    turn(0, fb)
    if paired:
        late_sends(upper == 1)
    if extra:

        @pl.when(long_me)
        def _():
            turn(fb, most)

    def fill(source, count):
        at = pl.ds(pl.multiple_of(source * sta_dev, sta_dev), sta_dev)
        for f in range(count):
            re = blocks[source, 0, f].astype(f32)
            im = blocks[source, 1, f].astype(f32)
            c0 = rotor[f, 0, 2:3, at]
            s0 = rotor[f, 1, 2:3, at]
            parts = (re * c0 - im * s0, im * c0 + re * s0)
            trig = (cos_b[f, :, at], sin_b[f, :, at])
            for p in range(2):
                for ri in range(2):
                    for g in range(0, segs, 2):
                        both = jnp.concatenate(
                            [parts[ri][g : g + 1] * trig[p], parts[ri][g + 1 : g + 2] * trig[p]], 0
                        )
                        base = ((p * 2 + ri) * segs + g) * 8
                        left[f, base : base + 16, :] = both.astype(bf16)
            product[f] += lax.dot_general(
                left[f], turned[f, at, :], (((1,), (0,)), ((), ())), preferred_element_type=f32
            )

    def whiten(source, count):
        scale_arrival(source).wait_recv()
        factor = scales[source]
        for f in range(count):
            for c in range(2):
                blocks[source, c, f] = (blocks[source, c, f].astype(f32) * factor).astype(bf16)

    def take(k, count, may_be_raw):
        source = jnp.where(k == 0, me, origin(k - 1))

        @pl.when(k > 0)
        def _():
            block_arrival(source, count).wait_recv()

        if may_be_raw:

            @pl.when(jnp.logical_and(k > 0, is_raw(source)))
            def _():
                whiten(source, count)

        fill(source, count)

    def arrive_step(k, carry):
        if not extra:
            take(k, fb, raw > 0)
            return carry

        @pl.when(long_me)
        def _():
            take(k, most, True)

        @pl.when(jnp.logical_not(long_me))
        def _():
            take(k, fb, True)

        return carry

    lax.fori_loop(0, n_sta, arrive_step, 0)

    part = segs * 8

    def bin_power(f, carry):
        sums = [None] * 4
        for g in range(segs):
            r0 = g * 8
            ccr, csr = product[f, r0 : r0 + 8, :128], product[f, r0 : r0 + 8, 128:]
            r0 += part
            cci, csi = product[f, r0 : r0 + 8, :128], product[f, r0 : r0 + 8, 128:]
            r0 += part
            scr, ssr = product[f, r0 : r0 + 8, :128], product[f, r0 : r0 + 8, 128:]
            r0 += part
            sci, ssi = product[f, r0 : r0 + 8, :128], product[f, r0 : r0 + 8, 128:]
            pr, pi, mr, mi = ccr - ssr, cci - ssi, ccr + ssr, cci + ssi
            tr, ti, dr, di = scr + csr, sci + csi, scr - csr, sci - csi
            amps = (
                (pr + ti, pi - tr),
                (mr + di, mi - dr),
                (mr - di, mi + dr),
                (pr - ti, pi + tr),
            )
            for c, (x, y) in enumerate(amps):
                power = x * x + y * y
                sums[c] = power if sums[c] is None else sums[c] + power
        grid = jnp.concatenate(
            [jnp.concatenate(sums[0:2], 1), jnp.concatenate(sums[2:4], 1)], 0
        )
        hi = grid.astype(bf16)
        lo = (grid - hi.astype(f32)).astype(bf16)
        grid_hi_lo[0, f] = hi
        grid_hi_lo[1, f] = lo
        return carry

    lax.fori_loop(0, bins_me if extra else most, bin_power, 0)

    rows = jnp.concatenate(
        [grid_hi_lo[h, f] for h in range(2) for f in range(most)], 0
    )

    def result_send(there):
        return pltpu.make_async_remote_copy(
            src_ref=picked.at[there],
            dst_ref=returned.at[group],
            send_sem=re_send,
            recv_sem=re_recv,
            device_id={"sta": there * copies + lane_of},
            device_id_type=MESH,
        )

    def results_of(count):
        return pltpu.make_async_remote_copy(
            src_ref=returned.at[pl.ds(0, count)],
            dst_ref=returned.at[pl.ds(0, count)],
            send_sem=re_send,
            recv_sem=re_recv,
            device_id={"sta": me},
            device_id_type=MESH,
        )

    packed_rows = 16 * most
    def pick(there):
        if copies == 1:
            at = pl.ds(there * beams_dev, beams_dev)
        else:
            target = there * copies + lane_of
            at = pl.ds(pl.multiple_of(target * beams_dev, beams_dev), beams_dev)
        values = jnp.dot(rows, onehot[:, at], preferred_element_type=f32)
        values = values[:packed_rows] + values[packed_rows:]
        for f in range(most):
            line = jnp.sum(values[f * 16 : (f + 1) * 16] * keep[:, at], axis=0, keepdims=True)
            picked[there, f : f + 1, :] = line

    soon = min(2, groups)
    for span in (range(soon), range(soon, groups)):
        for there in span:
            pick(there)
        for there in span:

            @pl.when(there != group)
            def _():
                result_send(there).start()

    returned[group] = picked[group]

    if groups > 1:
        results_of(groups - 1).wait_recv()
    for g in range(groups):
        count = most if not extra or g < half else fb
        begin = g * most - max(g - half, 0) * extra
        out[begin : begin + count, :] = returned[g, :count]

    if n_bins > 1:
        squares_of(n_bins - 1).wait_send()
    if n_sta > 1:
        blocks_sent()
    for k in range(raw):

        @pl.when(sent_raw(k))
        def _():
            scales_of(1).wait_send()

    if groups > 1:
        results_of(groups - 1).wait_send()


def solution(mesh):
    n_bins, n_sta = mesh.shape["bins"], mesh.shape["sta"]

    def local(spectra, coords, slowness):
        _, bins_dev, segs, sta_dev = spectra.shape
        stations, beams = coords.shape[1], slowness.shape[1]
        beams_dev = beams // n_sta
        groups = math.gcd(bins_dev, n_sta)
        copies = n_sta // groups
        fb = bins_dev // groups
        extra = 0
        if copies == 1 and n_sta >= 4 and n_sta & (n_sta - 1) == 0 and fb >= 4:
            extra = 2 * (fb // 4)
            fb = fb - fb // 4
        most = fb + extra
        dims = (n_bins, n_sta, groups, copies, fb, extra, bins_dev, segs, sta_dev, beams_dev)
        f32, bf16 = jnp.float32, jnp.bfloat16
        dma = pltpu.SemaphoreType.DMA
        return pl.pallas_call(
            functools.partial(kernel, dims),
            out_shape=pltpu.VMEM((bins_dev, beams_dev), f32),
            in_specs=[
                pl.BlockSpec(memory_space=pltpu.HBM),
                pl.BlockSpec(memory_space=pltpu.HBM),
                pl.BlockSpec(memory_space=pltpu.HBM),
            ],
            out_specs=pl.BlockSpec(memory_space=pltpu.VMEM),
            scratch_shapes=[
                pltpu.VMEM((2, stations), jnp.int32),
                pltpu.VMEM((2, beams), jnp.int32),
                pltpu.VMEM((2, bins_dev, segs, sta_dev), bf16),
                pltpu.VMEM((2, bins_dev, segs, sta_dev), bf16),
                pltpu.VMEM((n_sta, 2, most, segs, sta_dev), bf16),
                pltpu.VMEM((n_bins, segs, sta_dev), f32),
                pltpu.VMEM((n_sta, segs, sta_dev), f32),
                pltpu.VMEM((most, 8, stations), f32),
                pltpu.VMEM((most, 8, stations), f32),
                pltpu.VMEM((most, 2, 8, stations), f32),
                pltpu.VMEM((most, 256, stations), bf16),
                pltpu.VMEM((most, stations, 256), bf16),
                pltpu.VMEM((most, 32 * segs, sta_dev), bf16),
                pltpu.VMEM((most, 32 * segs, 256), f32),
                pltpu.VMEM((2, most, 16, 256), bf16),
                pltpu.VMEM((256, beams), bf16),
                pltpu.VMEM((16, beams), f32),
                pltpu.VMEM((n_sta, most, beams_dev), f32),
                pltpu.VMEM((groups, most, beams_dev), f32),
                pltpu.SemaphoreType.REGULAR((n_sta,)),
                dma,
                dma,
                dma,
                dma,
                dma,
                dma,
                dma((max(1, n_sta // 2),)),
                dma,
                dma((n_sta,)),
                dma,
                dma,
            ],
            compiler_params=pltpu.CompilerParams(
                collective_id=0,
                has_side_effects=True,
                vmem_limit_bytes=33554432,
            ),
            name="beam_power",
        )(*(pltpu.with_memory_space_constraint(x, pltpu.HBM) for x in (spectra, coords, slowness)))

    in_specs = (P(None, "bins", None, "sta"), P(), P())
    out_specs = P("bins", "sta")
    return jax.shard_map(local, mesh=mesh, in_specs=in_specs, out_specs=out_specs, check_vma=False)
```

```python
import functools
import math

import jax
import jax.numpy as jnp
from jax import lax
from jax.experimental import pallas as pl
from jax.experimental.pallas import tpu as pltpu
from jax.sharding import PartitionSpec as P

epsilon = 1e-06
MESH = pl.DeviceIdType.MESH

SIN_COEFS = (6.28318501, -41.3415909, 81.5999451, -76.6144714, 41.3428841, -12.4712439)
COS_COEFS = (1.0, -19.7392044, 64.9391174, -85.4501419, 60.1676292, -25.9675999, 6.52865839)


def horner(coefs, z):
    acc = jnp.full_like(z, coefs[-1])
    for c in coefs[-2::-1]:
        acc = acc * z + c
    return acc


def cos_sin(index):
    turns = (index << 11).astype(jnp.float32) * (2.0 ** -32)
    z = turns * turns
    return horner(COS_COEFS, z), horner(SIN_COEFS, z) * turns


def kernel(
    dims,
    spectra,
    coords_hbm,
    slowness_hbm,
    out,
    coords,
    slowness,
    own,
    white,
    blocks,
    squares,
    scales,
    cos_b,
    sin_b,
    rotor,
    right,
    turned,
    left,
    product,
    grid_hi_lo,
    onehot,
    keep,
    picked,
    returned,
    entered,
    own_sem,
    coords_sem,
    slow_sem,
    sq_send,
    sq_recv,
    sc_send,
    sc_recv,
    bl_send,
    bl_recv,
    re_send,
    re_recv,
):
    n_bins, n_sta, groups, copies, fb, extra, bins_dev, segs, sta_dev, beams_dev = dims
    me = lax.axis_index("sta")
    mb = lax.axis_index("bins")
    group = me // copies
    lane_of = me % copies
    f32, bf16 = jnp.float32, jnp.bfloat16
    most = fb + extra

    paired = n_sta >= 4 and n_sta & (n_sta - 1) == 0
    half = n_sta // 2
    upper = me // half if paired else 0

    edge = n_sta // 4
    raw = 2 if paired else 0

    def partner(k):
        if not paired:
            return (me + k + 1) % n_sta
        flip = me & 1
        if k < 2:
            early = half - 2 + k
        elif k < half:
            early = me ^ k ^ flip
        elif k < n_sta - 2:
            early = k - half
        else:
            early = me ^ 1 ^ flip
        if k < half:
            late = half + k if half < 4 else ((half, n_sta - 2, n_sta - 1)[k] if k < 3 else half + k - 2)
            across = me + edge
            rest = n_sta - k
            rest = across if k == 0 else rest - jnp.where(rest <= across, 1, 0)
            if k in (1, 2) and half >= 4:
                rest = rest ^ (1 - flip)
            late = jnp.where(me < edge, late, rest ^ flip)
        else:
            late = me ^ (k - half + 2 if k < n_sta - 2 else 1) ^ flip
        return jnp.where(upper == 1, early, late) ^ flip

    def origin(k):
        if not paired:
            return (me - k - 1 + n_sta) % n_sta
        outer = k - (half - 1)
        spread = half + outer
        if half >= 4:
            spread = jnp.where(outer == 0, half, n_sta - 3 + outer)
            spread = jnp.where(outer > 2, half + outer - 2, spread)
        at_edge = jnp.where(outer < 0, me ^ (k + 1), spread ^ (me & 1))
        at_inner = jnp.where(k < half, half + k, me ^ (k - half + 1))
        side = me & 1
        at_upper = jnp.where(k == 0, me ^ 1, k - 1)
        if half >= 4:
            cross = 2 * (n_sta - 2 - k) + 1 - side
            at_upper = jnp.where(k < half + half // 2 - 1, me ^ (k - half // 2 + 1), cross)
            at_upper = jnp.where(k < half // 2 + 2, 2 * (k - 2) + side, at_upper)
            at_upper = jnp.where(k < 2, me ^ (k + 1), at_upper)
        return jnp.where(upper == 1, at_upper, jnp.where(me < edge, at_edge, at_inner))

    def first_of(part):
        if extra:
            return part * most - jnp.maximum(part - half, 0) * extra
        return part * fb

    def is_long(part):
        return part < half

    long_me = is_long(group)
    bins_me = jnp.where(long_me, most, fb)
    first_me = first_of(group)
    prompt = mb % 2 == 0

    inner = jnp.logical_and(me >= edge, me < half)

    def sent_raw(k):
        if not raw or k >= raw:
            return False
        return jnp.logical_or(upper == 1, inner) if k == 0 else upper == 1

    def is_raw(source):
        from_far = jnp.logical_and(
            source // half == 1, jnp.logical_and(me >= half - 2, me < half)
        )
        from_near = jnp.logical_and(
            source == me - edge, jnp.logical_and(me >= half, me < half + edge)
        )
        return jnp.logical_or(from_far, from_near)

    def scale_slot(source):
        return jnp.maximum(source - half, 0)

    own_copy = pltpu.make_async_copy(spectra, own, own_sem)
    own_copy.start()
    coords_copy = pltpu.make_async_copy(coords_hbm, coords, coords_sem)
    coords_copy.start()
    slow_copy = pltpu.make_async_copy(slowness_hbm, slowness, slow_sem)
    slow_copy.start()

    barrier = pltpu.get_barrier_semaphore()
    for o in range(1, n_bins):
        pl.semaphore_signal(
            barrier, inc=1, device_id={"bins": (mb + o) % n_bins}, device_id_type=MESH
        )
    for o in range(1, n_sta):
        later = me + o

        @pl.when(later < n_sta)
        def _():
            pl.semaphore_signal(
                barrier, inc=1, device_id={"sta": later}, device_id_type=MESH
            )

    own_copy.wait()

    def square_step(f, acc):
        re = own[0, f].astype(f32)
        im = own[1, f].astype(f32)
        return acc + re * re + im * im

    squares[mb] = lax.fori_loop(
        0, bins_dev, square_step, jnp.zeros((segs, sta_dev), f32), unroll=True
    )

    pl.semaphore_wait(barrier, n_bins - 1 + me)
    for o in range(1, n_sta):
        earlier = me - o

        @pl.when(earlier >= 0)
        def _():
            pl.semaphore_signal(
                entered.at[me], inc=1, device_id={"sta": earlier}, device_id_type=MESH
            )


    def square_send(o):
        return pltpu.make_async_remote_copy(
            src_ref=squares.at[mb],
            dst_ref=squares.at[mb],
            send_sem=sq_send,
            recv_sem=sq_recv,
            device_id={"bins": (mb + o) % n_bins},
            device_id_type=MESH,
        )

    def squares_of(count):
        return pltpu.make_async_remote_copy(
            src_ref=squares.at[pl.ds(0, count)],
            dst_ref=squares.at[pl.ds(0, count)],
            send_sem=sq_send,
            recv_sem=sq_recv,
            device_id={"bins": mb},
            device_id_type=MESH,
        )

    def scale_send(k):
        return pltpu.make_async_remote_copy(
            src_ref=scales.at[me],
            dst_ref=scales.at[me],
            send_sem=sc_send,
            recv_sem=sc_recv.at[scale_slot(me)],
            device_id={"sta": partner(k)},
            device_id_type=MESH,
        )

    def scale_arrival(source):
        return pltpu.make_async_remote_copy(
            src_ref=scales.at[source],
            dst_ref=scales.at[source],
            send_sem=sc_send,
            recv_sem=sc_recv.at[scale_slot(source)],
            device_id={"sta": source},
            device_id_type=MESH,
        )

    def block_copy(k, values, begin, count):
        target = partner(k)
        return pltpu.make_async_remote_copy(
            src_ref=values.at[:, pl.ds(first_of(target // copies) + begin, count)],
            dst_ref=blocks.at[me, :, pl.ds(begin, count)],
            send_sem=bl_send,
            recv_sem=bl_recv.at[me],
            device_id={"sta": target},
            device_id_type=MESH,
        )

    def block_send(k, values):
        block_copy(k, values, 0, fb).start()
        if extra:

            @pl.when(is_long(partner(k)))
            def _():
                block_copy(k, values, fb, extra).start()

    def blocks_sent():
        def wait(ref):
            pltpu.make_async_remote_copy(
                src_ref=ref,
                dst_ref=ref,
                send_sem=bl_send,
                recv_sem=bl_recv.at[me],
                device_id={"sta": me},
                device_id_type=MESH,
            ).wait_send()

        if not extra:
            wait(blocks.at[pl.ds(0, n_sta - 1)])
            return

        @pl.when(long_me)
        def _():
            wait(white.at[:, pl.ds(0, bins_dev - most)])

        @pl.when(jnp.logical_not(long_me))
        def _():
            wait(white.at[:, pl.ds(0, bins_dev - fb)])

    def scales_of(count):
        return pltpu.make_async_remote_copy(
            src_ref=scales.at[pl.ds(0, count)],
            dst_ref=scales.at[pl.ds(0, count)],
            send_sem=sc_send,
            recv_sem=sc_recv.at[0],
            device_id={"sta": me},
            device_id_type=MESH,
        )

    def await_entry(k):
        target = partner(k)

        @pl.when(target > me)
        def _():
            pl.semaphore_wait(entered.at[target], 1)

    def block_arrival(source, count):
        return pltpu.make_async_remote_copy(
            src_ref=blocks.at[source, :, pl.ds(0, count)],
            dst_ref=blocks.at[source, :, pl.ds(0, count)],
            send_sem=bl_send,
            recv_sem=bl_recv.at[source],
            device_id={"sta": source},
            device_id_type=MESH,
        )

    for o in range(1, n_bins):
        square_send(o).start()
    def raw_sends(when):
        for k in range(raw):

            @pl.when(jnp.logical_and(sent_raw(k), when))
            def _():
                await_entry(k)
                block_send(k, own)

    raw_sends(upper == 1)

    coords_copy.wait()
    first_bin = mb * bins_dev + first_me + 1

    def table_step(step, carry):
        f = step // n_sta
        at = pl.ds(pl.multiple_of((step % n_sta) * sta_dev, sta_dev), sta_dev)
        bin_number = first_bin + f
        east = coords[0:1, at] * bin_number
        north = coords[1:2, at] * bin_number
        ids = lax.broadcasted_iota(jnp.int32, (8, sta_dev), 0)
        cb, sb = cos_sin((2 * ids + 1) * east)
        cos_b[f, :, at] = cb
        sin_b[f, :, at] = sb
        steps = jnp.where(ids == 0, 16, jnp.where(ids == 1, 48, 1))
        ca, sa = cos_sin(steps * east + jnp.where(ids == 2, north, 0))
        rotor[f, 0, :, at] = ca
        rotor[f, 1, :, at] = sa
        ids = lax.broadcasted_iota(jnp.int32, (16, sta_dev), 0)
        for half in range(2):
            cy, sy = cos_sin((2 * ids + (32 * half + 1)) * north)
            for a in range(2):
                c, s = ca[a : a + 1], sa[a : a + 1]
                cc, ss, sc, cs = c * cy, s * sy, s * cy, c * sy
                base = a * 64 + half * 16
                right[f, base : base + 16, at] = (cc - ss).astype(bf16)
                right[f, base + 32 : base + 48, at] = (cc + ss).astype(bf16)
                right[f, base + 128 : base + 144, at] = (sc + cs).astype(bf16)
                right[f, base + 160 : base + 176, at] = (sc - cs).astype(bf16)
        return carry

    most_steps = fb * n_sta - fb * n_sta // 4
    lax.fori_loop(0, most_steps, table_step, 0)
    raw_sends(inner)
    lax.fori_loop(most_steps, fb * n_sta, table_step, 0)

    product[...] = jnp.zeros_like(product)
    slow_copy.wait()
    sx = slowness[0:1, :] + 32
    sy = slowness[1:2, :] + 32
    a_index = sx // 16
    flipped = a_index < 2
    y_index = jnp.where(flipped, 63 - sy, sy)
    y_slot = jnp.where(y_index >= 32, y_index - 32, 63 - y_index)
    a_slot = jnp.where(flipped, 1 - a_index, a_index - 2)
    column = jnp.where(flipped, 128, 0) + a_slot * 64 + y_slot
    for i in range(16):
        ids = lax.broadcasted_iota(jnp.int32, (16, column.shape[1]), 0) + 16 * i
        onehot[i * 16 : (i + 1) * 16, :] = jnp.where(ids == column, 1.0, 0.0).astype(bf16)
    norm = 1.0 / (n_sta * sta_dev * segs)
    b_index = sx % 16
    row = jnp.where(b_index >= 8, b_index - 8, 15 - b_index)
    ids = lax.broadcasted_iota(jnp.int32, (16, column.shape[1]), 0)
    keep[...] = jnp.where(ids == row, norm, 0.0)


    if n_bins > 1:
        squares_of(n_bins - 1).wait_recv()
    total = squares[0]
    for b in range(1, n_bins):
        total = total + squares[b]
    inverse = 1.0 / jnp.sqrt(total / (2 * bins_dev * n_bins) + epsilon)
    scales[me] = inverse
    for f in range(bins_dev):
        for c in range(2):
            white[c, f] = (own[c, f].astype(f32) * inverse).astype(bf16)
    for k in range(raw):

        @pl.when(sent_raw(k))
        def _():
            scale_send(k).start()

    def crosses(k):
        late_far = 1 if k < half else 0
        early_far = 1 if half <= k < n_sta - 2 else 0
        return jnp.where(upper == 1, early_far, late_far) == 1

    def white_send(k, wanted):
        if k < raw:
            wanted = jnp.logical_and(wanted, jnp.logical_not(sent_raw(k)))

        @pl.when(wanted)
        def _():
            await_entry(k)
            block_send(k, white)

    for k in range(n_sta - 1):
        if paired:
            white_send(k, jnp.logical_or(prompt, jnp.logical_not(crosses(k))))
        else:
            white_send(k, True)

    for f in range(fb):
        for c in range(2):
            blocks[me, c, f] = white[c, first_me + f]
    if extra:

        @pl.when(long_me)
        def _():
            for f in range(fb, most):
                for c in range(2):
                    blocks[me, c, f] = white[c, first_me + f]

    if extra:
        lax.fori_loop(fb * n_sta, bins_me * n_sta, table_step, 0)
    def turn(begin, end):
        def turn_step(step, carry):
            at = pl.ds(pl.multiple_of(step * sta_dev, sta_dev), sta_dev)
            for f in range(begin, end):
                turned[f, at, :] = right[f, :, at].T
            return carry

        lax.fori_loop(0, n_sta, turn_step, 0)

    def late_sends(when):
        for k in range(n_sta - 2):
            white_send(k, jnp.logical_and(jnp.logical_and(jnp.logical_not(prompt), when), crosses(k)))

    if paired:
        late_sends(upper == 0)
    turn(0, fb)
    if paired:
        late_sends(upper == 1)
    if extra:

        @pl.when(long_me)
        def _():
            turn(fb, most)

    def fill(source, count):
        at = pl.ds(pl.multiple_of(source * sta_dev, sta_dev), sta_dev)
        for f in range(count):
            re = blocks[source, 0, f].astype(f32)
            im = blocks[source, 1, f].astype(f32)
            c0 = rotor[f, 0, 2:3, at]
            s0 = rotor[f, 1, 2:3, at]
            parts = (re * c0 - im * s0, im * c0 + re * s0)
            trig = (cos_b[f, :, at], sin_b[f, :, at])
            for p in range(2):
                for ri in range(2):
                    for g in range(0, segs, 2):
                        both = jnp.concatenate(
                            [parts[ri][g : g + 1] * trig[p], parts[ri][g + 1 : g + 2] * trig[p]], 0
                        )
                        base = ((p * 2 + ri) * segs + g) * 8
                        left[f, base : base + 16, :] = both.astype(bf16)
            product[f] += lax.dot_general(
                left[f], turned[f, at, :], (((1,), (0,)), ((), ())), preferred_element_type=f32
            )

    def whiten(source, count):
        scale_arrival(source).wait_recv()
        factor = scales[source]
        for f in range(count):
            for c in range(2):
                blocks[source, c, f] = (blocks[source, c, f].astype(f32) * factor).astype(bf16)

    def take(k, count, may_be_raw):
        source = jnp.where(k == 0, me, origin(k - 1))

        @pl.when(k > 0)
        def _():
            block_arrival(source, count).wait_recv()

        if may_be_raw:

            @pl.when(jnp.logical_and(k > 0, is_raw(source)))
            def _():
                whiten(source, count)

        fill(source, count)

    def arrive_step(k, carry):
        if not extra:
            take(k, fb, raw > 0)
            return carry

        @pl.when(long_me)
        def _():
            take(k, most, True)

        @pl.when(jnp.logical_not(long_me))
        def _():
            take(k, fb, True)

        return carry

    lax.fori_loop(0, n_sta, arrive_step, 0)

    part = segs * 8

    def bin_power(f, carry):
        sums = [None] * 4
        for g in range(segs):
            r0 = g * 8
            ccr, csr = product[f, r0 : r0 + 8, :128], product[f, r0 : r0 + 8, 128:]
            r0 += part
            cci, csi = product[f, r0 : r0 + 8, :128], product[f, r0 : r0 + 8, 128:]
            r0 += part
            scr, ssr = product[f, r0 : r0 + 8, :128], product[f, r0 : r0 + 8, 128:]
            r0 += part
            sci, ssi = product[f, r0 : r0 + 8, :128], product[f, r0 : r0 + 8, 128:]
            pr, pi, mr, mi = ccr - ssr, cci - ssi, ccr + ssr, cci + ssi
            tr, ti, dr, di = scr + csr, sci + csi, scr - csr, sci - csi
            amps = (
                (pr + ti, pi - tr),
                (mr + di, mi - dr),
                (mr - di, mi + dr),
                (pr - ti, pi + tr),
            )
            for c, (x, y) in enumerate(amps):
                power = x * x + y * y
                sums[c] = power if sums[c] is None else sums[c] + power
        grid = jnp.concatenate(
            [jnp.concatenate(sums[0:2], 1), jnp.concatenate(sums[2:4], 1)], 0
        )
        hi = grid.astype(bf16)
        lo = (grid - hi.astype(f32)).astype(bf16)
        grid_hi_lo[0, f] = hi
        grid_hi_lo[1, f] = lo
        return carry

    lax.fori_loop(0, bins_me if extra else most, bin_power, 0)

    rows = jnp.concatenate(
        [grid_hi_lo[h, f] for h in range(2) for f in range(most)], 0
    )

    def result_send(there):
        return pltpu.make_async_remote_copy(
            src_ref=picked.at[there],
            dst_ref=returned.at[group],
            send_sem=re_send,
            recv_sem=re_recv,
            device_id={"sta": there * copies + lane_of},
            device_id_type=MESH,
        )

    def results_of(count):
        return pltpu.make_async_remote_copy(
            src_ref=returned.at[pl.ds(0, count)],
            dst_ref=returned.at[pl.ds(0, count)],
            send_sem=re_send,
            recv_sem=re_recv,
            device_id={"sta": me},
            device_id_type=MESH,
        )

    packed_rows = 16 * most
    def pick(there):
        if copies == 1:
            at = pl.ds(there * beams_dev, beams_dev)
        else:
            target = there * copies + lane_of
            at = pl.ds(pl.multiple_of(target * beams_dev, beams_dev), beams_dev)
        values = jnp.dot(rows, onehot[:, at], preferred_element_type=f32)
        values = values[:packed_rows] + values[packed_rows:]
        for f in range(most):
            line = jnp.sum(values[f * 16 : (f + 1) * 16] * keep[:, at], axis=0, keepdims=True)
            picked[there, f : f + 1, :] = line

    soon = min(2, groups)
    for span in (range(soon), range(soon, groups)):
        for there in span:
            pick(there)
        for there in span:

            @pl.when(there != group)
            def _():
                result_send(there).start()

    returned[group] = picked[group]

    if groups > 1:
        results_of(groups - 1).wait_recv()
    for g in range(groups):
        count = most if not extra or g < half else fb
        begin = g * most - max(g - half, 0) * extra
        out[begin : begin + count, :] = returned[g, :count]

    if n_bins > 1:
        squares_of(n_bins - 1).wait_send()
    if n_sta > 1:
        blocks_sent()
    for k in range(raw):

        @pl.when(sent_raw(k))
        def _():
            scales_of(1).wait_send()

    if groups > 1:
        results_of(groups - 1).wait_send()


def solution(mesh):
    n_bins, n_sta = mesh.shape["bins"], mesh.shape["sta"]

    def local(spectra, coords, slowness):
        _, bins_dev, segs, sta_dev = spectra.shape
        stations, beams = coords.shape[1], slowness.shape[1]
        beams_dev = beams // n_sta
        groups = math.gcd(bins_dev, n_sta)
        copies = n_sta // groups
        fb = bins_dev // groups
        extra = 0
        if copies == 1 and n_sta >= 4 and n_sta & (n_sta - 1) == 0 and fb >= 4:
            extra = 2 * (fb // 4)
            fb = fb - fb // 4
        most = fb + extra
        dims = (n_bins, n_sta, groups, copies, fb, extra, bins_dev, segs, sta_dev, beams_dev)
        f32, bf16 = jnp.float32, jnp.bfloat16
        dma = pltpu.SemaphoreType.DMA
        return pl.pallas_call(
            functools.partial(kernel, dims),
            out_shape=pltpu.VMEM((bins_dev, beams_dev), f32),
            in_specs=[
                pl.BlockSpec(memory_space=pltpu.HBM),
                pl.BlockSpec(memory_space=pltpu.HBM),
                pl.BlockSpec(memory_space=pltpu.HBM),
            ],
            out_specs=pl.BlockSpec(memory_space=pltpu.VMEM),
            scratch_shapes=[
                pltpu.VMEM((2, stations), jnp.int32),
                pltpu.VMEM((2, beams), jnp.int32),
                pltpu.VMEM((2, bins_dev, segs, sta_dev), bf16),
                pltpu.VMEM((2, bins_dev, segs, sta_dev), bf16),
                pltpu.VMEM((n_sta, 2, most, segs, sta_dev), bf16),
                pltpu.VMEM((n_bins, segs, sta_dev), f32),
                pltpu.VMEM((n_sta, segs, sta_dev), f32),
                pltpu.VMEM((most, 8, stations), f32),
                pltpu.VMEM((most, 8, stations), f32),
                pltpu.VMEM((most, 2, 8, stations), f32),
                pltpu.VMEM((most, 256, stations), bf16),
                pltpu.VMEM((most, stations, 256), bf16),
                pltpu.VMEM((most, 32 * segs, sta_dev), bf16),
                pltpu.VMEM((most, 32 * segs, 256), f32),
                pltpu.VMEM((2, most, 16, 256), bf16),
                pltpu.VMEM((256, beams), bf16),
                pltpu.VMEM((16, beams), f32),
                pltpu.VMEM((n_sta, most, beams_dev), f32),
                pltpu.VMEM((groups, most, beams_dev), f32),
                pltpu.SemaphoreType.REGULAR((n_sta,)),
                dma,
                dma,
                dma,
                dma,
                dma,
                dma,
                dma((max(1, n_sta // 2),)),
                dma,
                dma((n_sta,)),
                dma,
                dma,
            ],
            compiler_params=pltpu.CompilerParams(
                collective_id=0,
                has_side_effects=True,
                vmem_limit_bytes=33554432,
            ),
            name="beam_power",
        )(*(pltpu.with_memory_space_constraint(x, pltpu.HBM) for x in (spectra, coords, slowness)))

    in_specs = (P(None, "bins", None, "sta"), P(), P())
    out_specs = P("bins", "sta")
    return jax.shard_map(local, mesh=mesh, in_specs=in_specs, out_specs=out_specs, check_vma=False)
```
